32 devices in a mesh: space: 16 (over z, y, x), level: 2 (over core).
Axes of the slice: x: 2, y: 2, z: 4, core: 2. Of those that a mesh axis runs over, the one named last changes fastest.
Arguments:
- velocity: float32 [2, 16, 16384], P(None, 'level', 'space'), may hold values from -3 to 3
- density: float32 [16, 16384], P('level', 'space'), may hold values from -6 to 6
- elevation: float32 [16384], P('space'), may hold values from -3 to 3
- grad_weights: float32 [2, 6, 16384], P(None, None, 'space'), may hold values from -2.4 to 2.4
- lap_weights: float32 [6, 16384], P(None, 'space'), may hold values from 0.02 to 0.2
- coriolis: float32 [16384], P('space'), may hold values from 0.5 to 2
- node_area: float32 [16384], P('space'), may hold values from 1 to 100, as said below
- thickness: float32 [16], P('level'), may hold values from 0.5 to 2
- send_list: int32 [16, 256], P('space'), may hold values from 0 to 1023
- neighbours: int32 [6, 16384], P(None, 'space'), may hold values from 0 to 1279
- bottom: int32 [16384], P('space'), may hold values from 0 to 16, as said below
Outputs:
- velocity_out: float32 [2, 16, 16384], P(None, 'level', 'space')
- density_out: float32 [16, 16384], P('level', 'space')
- elevation_out: float32 [16384], P('space')
- volume_drift: float32 [4], replicated
The draws below stay inside these ranges and needn't reach their ends.
Inputs may be any that keep to these rules, and one draw needn't show every extreme that they name: `send_list`: local node numbers within the sending partition; the first 128 go to the partition one below along space, the other 128 to the one above. `neighbours`: slots below 1024 are the partition's own nodes; the next 128 are halo slots filled from the partition below, the last 128 from the partition above. Levels of a node are wet from the surface down to bottom - 1; a node with 0 is dry. Some partitions are shallower than others. `node_area`: positive areas.
All inputs are finite; a program needn't handle non-finite values.
Results may differ from the reference program's by a relative error of at most 0.00013.
Values sent between devices are 32-bit elements; how exact they have to be, the bound alone decides.
A program may use at most 64 MiB of HBM per device.

```python
import math
import jax
import jax.numpy as jnp
from jax import lax

NODES_DEV = 1024
HALO = 128
K = 6
STEPS = 4
NODES = 16384
LEVELS = 16
N_SPACE = 16


def draw_bottom(key, part):
    key_part = jax.random.fold_in(key, 11)
    key_node = jax.random.fold_in(key, 12)
    partitions = NODES // NODES_DEV
    shallow = jax.random.randint(key_part, (partitions, 1), LEVELS // 4, LEVELS + 1)
    shallow = shallow.at[0].set(LEVELS)
    depths = jax.random.randint(key_node, (partitions, NODES_DEV), 0, LEVELS + 1)
    return jnp.minimum(depths, shallow).reshape(NODES).astype(jnp.int32)


def draw_node_area(key, part):
    key_rough = jax.random.fold_in(key, 21)
    partitions = NODES // NODES_DEV
    owner = (jnp.arange(NODES, dtype=jnp.int32) // NODES_DEV).astype(jnp.float32)
    position = owner / jnp.float32(max(partitions - 1, 1))
    ramp = jnp.exp(jnp.log(jnp.float32(10.0)) * position)
    rough = jnp.exp(jax.random.uniform(key_rough, (NODES,), jnp.float32, 0.0, jnp.log(3.0)))
    return (ramp * rough).astype(jnp.float32)


def plant(values, rng, smallest, high):
    spot = [jax.random.randint(jax.random.fold_in(rng, axis), (), 0, length) for axis, length in enumerate(values.shape)]
    longest = values.shape.index(max(values.shape))
    neighbour = spot[:longest] + [(spot[longest] + 1) % values.shape[longest]] + spot[longest + 1:]
    return values.at[tuple(spot)].set(smallest).at[tuple(neighbour)].set(high)


def block_levels(rng, extent, pieces, smallest, top_value):
    loudness, own = 1.0, jax.random.fold_in(rng, 6)
    for dim, blocks in pieces:
        heights = jnp.exp(jax.random.uniform(jax.random.fold_in(own, dim), (blocks,), jnp.float32, smallest / len(pieces), top_value / len(pieces)))
        loudness = loudness * jnp.repeat(heights, extent[dim] // blocks).reshape([-1 if axis == dim else 1 for axis in range(len(extent))])
    return loudness


def scatter_about(rng, shape, width, most, shards=(), held_as=jnp.bfloat16):
    loudness = block_levels(rng, shape, shards, -0.22, 0.18) if shards else 1.0
    values = jax.random.normal(rng, shape, jnp.float32) * width * loudness
    return jnp.minimum(jnp.maximum(values, -most), most).astype(held_as)


def setup_inputs(seed: int = 0) -> dict:
    key_list = jax.random.split(jax.random.key(seed), 12)
    return {
        "velocity": scatter_about(key_list[0], (2, LEVELS, NODES), 0.5, 3.0, ((1, 2), (2, 16)), jnp.float32),
        "density": scatter_about(key_list[1], (LEVELS, NODES), 1.0, 6.0, ((0, 2), (1, 16)), jnp.float32),
        "elevation": scatter_about(key_list[2], (NODES,), 0.5, 3.0, ((0, 16),), jnp.float32),
        "grad_weights": scatter_about(key_list[3], (2, K, NODES), 0.4, 2.4, ((2, 16),), jnp.float32),
        "lap_weights": jnp.clip(jnp.exp(math.log(0.2) - 2.3025851 * jax.random.uniform(key_list[4], (K, NODES), jnp.float32) ** block_levels(key_list[4], (K, NODES), ((1, 16),), -0.2, 0.2)), 0.02, 0.2),
        "coriolis": jnp.clip(jnp.exp(math.log(2.0) - 1.3862944 * jax.random.uniform(key_list[5], (NODES,), jnp.float32) ** block_levels(key_list[5], (NODES,), ((0, 16),), -0.2, 0.2)), 0.5, 2.0),
        "node_area": draw_node_area(jax.random.fold_in(key_list[11], 71), 0),
        "thickness": jnp.clip(jnp.exp(math.log(2.0) - 1.3862944 * jax.random.uniform(key_list[7], (LEVELS,), jnp.float32) ** block_levels(key_list[7], (LEVELS,), ((0, 2),), -0.2, 0.2)), 0.5, 2.0),
        "send_list": plant(jax.random.randint(key_list[8], (N_SPACE, 2 * HALO), 0, NODES_DEV), jax.random.fold_in(key_list[8], 1), 0, NODES_DEV - 1).astype(jnp.int32),
        "neighbours": plant(jax.random.randint(key_list[9], (K, NODES), 0, NODES_DEV + 2 * HALO), jax.random.fold_in(key_list[9], 1), 0, (NODES_DEV + 2 * HALO) - 1).astype(jnp.int32),
        "bottom": draw_bottom(jax.random.fold_in(key_list[11], 71), 0),
    }


time_step = 0.1
buoyancy = 0.5
drag_rate = 0.5


def neighbour_table(send_list, neighbours):
    node_ids = jnp.arange(NODES, dtype=jnp.int32)
    owner = (node_ids // NODES_DEV)[None, :]
    slot_index = neighbours
    source_below = jnp.clip(owner - 1, 0, N_SPACE - 1)
    source_above = jnp.clip(owner + 1, 0, N_SPACE - 1)
    local_below = send_list[source_below, jnp.clip(HALO + slot_index - NODES_DEV, 0, 2 * HALO - 1)]
    local_above = send_list[source_above, jnp.clip(slot_index - NODES_DEV - HALO, 0, 2 * HALO - 1)]
    global_index = jnp.where(slot_index < NODES_DEV, owner * NODES_DEV + slot_index,
                             jnp.where(slot_index < NODES_DEV + HALO, source_below * NODES_DEV + local_below,
                                       source_above * NODES_DEV + local_above))
    is_valid = jnp.where(slot_index < NODES_DEV, True,
                         jnp.where(slot_index < NODES_DEV + HALO, owner >= 1, owner <= N_SPACE - 2))
    return global_index.astype(jnp.int32), is_valid.astype(jnp.float32)


def stencil(fields, global_index, weight):
    result = jnp.zeros_like(fields)
    for column in range(K):
        nearby = jnp.take(fields, global_index[column], axis=-1)
        result = result + weight[column] * (nearby - fields)
    return result


def reference(velocity, density, elevation, grad_weights, lap_weights, coriolis, node_area, thickness, send_list, neighbours, bottom):
    global_index, valid_float = neighbour_table(send_list, neighbours)
    east_weight = grad_weights[0] * valid_float
    north_weight = grad_weights[1] * valid_float
    smooth_weight = lap_weights * valid_float
    level_ids = jnp.arange(LEVELS, dtype=jnp.int32)[:, None]
    wet_cells = (level_ids < bottom[None, :]).astype(jnp.float32)
    at_floor = (level_ids == bottom[None, :] - 1).astype(jnp.float32)
    wet_nodes = (bottom > 0).astype(jnp.float32)
    area_total = jnp.sum(node_area * wet_nodes)
    velocity = velocity * wet_cells[None]
    drifts = []
    for counter in range(STEPS):
        east_speed = velocity[0]
        north_speed = velocity[1]
        weighted = density * thickness[:, None]
        pressure = buoyancy * (jnp.cumsum(weighted, axis=0) - 0.5 * weighted)
        transport = jnp.einsum('cln,l->cn', velocity, thickness, precision=lax.Precision.HIGHEST)
        diverge = stencil(transport[0], global_index, east_weight) + stencil(transport[1], global_index, north_weight)
        drift = jnp.sum(node_area * wet_nodes * diverge) / area_total
        drifts.append(drift)
        new_elevation = elevation - time_step * wet_nodes * diverge + time_step * drift
        slope_east = stencil(elevation, global_index, east_weight)
        slope_north = stencil(elevation, global_index, north_weight)
        press_east = stencil(pressure, global_index, east_weight)
        press_north = stencil(pressure, global_index, north_weight)
        smooth_speed = stencil(velocity.reshape(2 * LEVELS, NODES), global_index, smooth_weight)
        push_east = (-slope_east[None] - press_east + coriolis[None] * north_speed
                     + smooth_speed[:LEVELS] - drag_rate * at_floor * east_speed)
        push_north = (-slope_north[None] - press_north - coriolis[None] * east_speed
                      + smooth_speed[LEVELS:] - drag_rate * at_floor * north_speed)
        dense_east = stencil(density, global_index, east_weight)
        dense_north = stencil(density, global_index, north_weight)
        dense_smooth = stencil(density, global_index, smooth_weight)
        density = density + time_step * (dense_smooth - east_speed * dense_east - north_speed * dense_north)
        velocity = wet_cells[None] * (velocity + time_step * jnp.stack([push_east, push_north]))
        elevation = new_elevation
    return velocity, density, elevation, jnp.stack(drifts).astype(jnp.float32)
```

```python
import functools

import jax
import jax.numpy as jnp
from jax import lax
from jax.experimental import pallas as pl
from jax.experimental.pallas import tpu as pltpu
from jax.sharding import PartitionSpec as P

STEPS = 4
LANES = 128

time_step = 0.1
buoyancy = 0.5
drag_rate = 0.5


def lane_gather(values, lanes):
    return jnp.take_along_axis(values, lanes, axis=1, mode="promise_in_bounds")


def pick(tiles, lanes, masks):
    found = lane_gather(tiles[0], lanes)
    for tile, mask in zip(tiles[1:], masks):
        found = jnp.where(mask, lane_gather(tile, lanes), found)
    return found


def running_sum(values, rows, row_ids):
    shift = 1
    while shift < rows:
        moved = pltpu.roll(values, shift, 0)
        values = values + jnp.where(row_ids >= shift, moved, 0.0)
        shift *= 2
    return values


def kernel(
    n_space, n_level, rows, blocks, near_count,
    vel, den, ele, grad, lap, cor, area, thick, send, near, bot,
    vel_out, den_out, ele_out, drift_out,
    own, eta, lanes_of, block_of, east_of, north_of, smooth_of, flow_of,
    held, press, flow, small, out, halo, halo_small, peer,
    vol, vol_all,
    main_send, main_recv, hs_send, hs_recv, peer_send, peer_recv, vol_send, vol_recv,
):
    sp = lax.axis_index("space")
    lv = lax.axis_index("level")
    has = (sp > 0, sp < n_space - 1)
    ends = (sp - 1, sp + 1)

    barrier = pltpu.get_barrier_semaphore()

    def greet(d, _):
        pl.semaphore_signal(barrier, inc=1, device_id={"space": lax.rem(sp + d, n_space), "level": lv})
        return 0

    lax.fori_loop(1, n_space, greet, 0)
    for d in range(1, n_level):
        q = lax.rem(lv + d, n_level)
        pl.semaphore_signal(barrier, inc=1, device_id={"space": sp, "level": q})
        for side in range(2):
            @pl.when(has[side])
            def _():
                pl.semaphore_signal(barrier, inc=1, device_id={"space": ends[side], "level": q})

    row_ids = lax.broadcasted_iota(jnp.int32, (rows, LANES), 0)
    eight = lax.broadcasted_iota(jnp.int32, (8, LANES), 0)
    level_ids = row_ids + lv * rows
    thickness = jnp.zeros((rows, LANES), jnp.float32)
    for r in range(rows):
        thickness = jnp.where(row_ids == r, thick[r], thickness)

    def wide(row, count=rows):
        return jnp.broadcast_to(row, (count, LANES))

    low = jnp.where(has[0], 1, 0)
    high = jnp.where(has[1], 1, 0)

    def prepare(t, _):
        here = pl.ds(pl.multiple_of(t * LANES, LANES), LANES)
        bottom = wide(bot[pl.ds(t, 1), :])
        wet = level_ids < bottom
        own[0, t] = jnp.where(wet, vel[0, :, here], 0.0)
        own[1, t] = jnp.where(wet, vel[1, :, here], 0.0)
        own[2, t] = den[:, here]
        eta[t] = wide(ele[pl.ds(t, 1), :], 8)
        for k in range(near_count):
            slot = wide(near[k:k + 1, here])
            block = lax.shift_right_logical(slot, 7)
            inside = jnp.where(block < blocks, 1, jnp.where(block == blocks, low, high))
            valid = inside > 0
            lanes_of[t, k] = jnp.bitwise_and(slot, LANES - 1)
            block_of[t, k] = jnp.where(valid, block, 0)
            east = jnp.where(valid, wide(grad[0, k:k + 1, here]), 0.0)
            north = jnp.where(valid, wide(grad[1, k:k + 1, here]), 0.0)
            east_of[t, k] = east
            north_of[t, k] = north
            smooth_of[t, k] = jnp.where(valid, wide(lap[k:k + 1, here]), 0.0)
            flow_of[t, k] = jnp.where(eight == 0, east[:8], jnp.where(eight == 1, north[:8], 0.0))
        return 0

    lax.fori_loop(0, blocks, prepare, 0)
    wet_area = area[...] * jnp.where(bot[...] > 0, 1.0, 0.0)
    vol[...] = jnp.where(eight == STEPS, wide(jnp.sum(wet_area, axis=0, keepdims=True), 8), 0.0)

    def main_copy(s, side):
        return pltpu.make_async_remote_copy(
            src_ref=out.at[s, side], dst_ref=halo.at[s, 1 - side],
            send_sem=main_send.at[s, side], recv_sem=main_recv.at[s, 1 - side],
            device_id={"space": ends[side], "level": lv}, device_id_type=pl.DeviceIdType.MESH)

    def small_copy(s, side, q, slot):
        return pltpu.make_async_remote_copy(
            src_ref=out.at[s, side, pl.ds(3 * rows, 8)], dst_ref=halo_small.at[s, 1 - side, slot],
            send_sem=hs_send.at[s, side, q], recv_sem=hs_recv.at[s, 1 - side, slot],
            device_id={"space": ends[side], "level": q}, device_id_type=pl.DeviceIdType.MESH)

    def peer_copy(s, q, slot):
        return pltpu.make_async_remote_copy(
            src_ref=small.at[s], dst_ref=peer.at[s, slot],
            send_sem=peer_send.at[s, q], recv_sem=peer_recv.at[s, slot],
            device_id={"space": sp, "level": q}, device_id_type=pl.DeviceIdType.MESH)

    def vol_copy(q, slot):
        return pltpu.make_async_remote_copy(
            src_ref=vol, dst_ref=vol_all.at[slot],
            send_sem=vol_send.at[q], recv_sem=vol_recv.at[slot],
            device_id={"space": q, "level": lv}, device_id_type=pl.DeviceIdType.MESH)

    others = [lax.rem(lv + d, n_level) for d in range(1, n_level)]

    def make_small(s):
        def body(t, _):
            total = jnp.sum(own[2, t] * thickness, axis=0, keepdims=True)
            flow0 = jnp.sum(own[0, t] * thickness, axis=0, keepdims=True)
            flow1 = jnp.sum(own[1, t] * thickness, axis=0, keepdims=True)
            tile = jnp.where(eight == 0, wide(flow0, 8), jnp.where(eight == 1, wide(flow1, 8), 0.0))
            tile = jnp.where(eight == 2, wide(total, 8), tile)
            small[s, t] = jnp.where(eight == 3, eta[t], tile)
            return 0
        lax.fori_loop(0, blocks, body, 0, unroll=True)

    def send_out(s):
        for side in range(2):
            slot = wide(send[:, side * LANES:(side + 1) * LANES])
            lanes = jnp.bitwise_and(slot, LANES - 1)
            block = lax.shift_right_logical(slot, 7)
            masks = [block == b for b in range(1, blocks)]
            for g in range(3):
                out[s, side, g * rows:(g + 1) * rows] = pick([own[g, b] for b in range(blocks)], lanes, masks)
            out[s, side, 3 * rows:3 * rows + 8] = pick(
                [small[s, b] for b in range(blocks)], lanes[:8], [m[:8] for m in masks])
        for q in others:
            peer_copy(s, q, lv).start()
        for side in range(2):
            @pl.when(has[side])
            def _():
                for q in others:
                    small_copy(s, side, q, lv).start()
                main_copy(s, side).start()

    def gather_own():
        def body(t, _):
            tiles = [[own[g, b] for b in range(blocks)] for g in range(3)]
            for k in range(near_count):
                lanes = lanes_of[t, k]
                block = block_of[t, k]
                masks = [block == b for b in range(1, blocks)]
                for g in range(3):
                    held[t, k, g] = pick(tiles[g], lanes, masks)
            return 0
        lax.fori_loop(0, blocks, body, 0)

    def receive(s):
        for q in others:
            peer_copy(s, q, q).wait_recv()
        for side in range(2):
            @pl.when(has[side])
            def _():
                main_copy(s, 1 - side).wait_recv()
                for q in others:
                    small_copy(s, 1 - side, q, q).wait_recv()

    def close(s):
        for q in others:
            peer_copy(s, q, lv).wait_send()
        for side in range(2):
            @pl.when(has[side])
            def _():
                main_copy(s, side).wait_send()
                for q in others:
                    small_copy(s, side, q, lv).wait_send()

    def columns(s):
        def finish(slot, density, mine, pieces):
            above = jnp.zeros((1, LANES), jnp.float32)
            total = mine
            for q, piece in zip(others, pieces):
                total = total + piece
                above = above + jnp.where(q < lv, piece[2:3], 0.0)
            weighted = density * thickness
            column = wide(above) + running_sum(weighted, rows, row_ids) - 0.5 * weighted
            press[slot] = wide(mine[3:4]) + buoyancy * column
            flow[slot] = total

        def body(t, _):
            finish(t, own[2, t], small[s, t], [peer[s, q, t] for q in others])
            return 0
        lax.fori_loop(0, blocks, body, 0, unroll=True)
        for side in range(2):
            finish(blocks + side, halo[s, side, 2 * rows:3 * rows], halo[s, side, 3 * rows:3 * rows + 8],
                   [halo_small[s, side, q] for q in others])

    def surface(s):
        tiles = [flow[b] for b in range(blocks + 2)]

        def body(t, volume):
            middle = flow[t]
            total = jnp.zeros((8, LANES), jnp.float32)
            for k in range(near_count):
                block = block_of[t, k][:8]
                masks = [block == b for b in range(1, blocks + 2)]
                found = pick(tiles, lanes_of[t, k][:8], masks)
                total = total + flow_of[t, k] * jnp.where(eight < 2, found - middle, 0.0)
            diverge = jnp.sum(total, axis=0, keepdims=True)
            wet_node = jnp.where(bot[pl.ds(t, 1), :] > 0, 1.0, 0.0)
            part = wet_node * diverge
            eta[t] = eta[t] - time_step * wide(part, 8)
            return volume + area[pl.ds(t, 1), :] * part

        volume = lax.fori_loop(0, blocks, body, jnp.zeros((1, LANES), jnp.float32))
        vol[...] = jnp.where(eight == s, wide(volume, 8), vol[...])

    def advance(s):
        pressures = [press[b] for b in range(blocks + 2)]
        edges = [[halo[s, side, g * rows:(g + 1) * rows] for side in range(2)] for g in range(3)]

        def body(t, _):
            here = [own[0, t], own[1, t], own[2, t], press[t]]
            zero = jnp.zeros((rows, LANES), jnp.float32)
            lap0 = lap1 = lap2 = east2 = north2 = east3 = north3 = zero
            for k in range(near_count):
                lanes = lanes_of[t, k]
                block = block_of[t, k]
                masks = [block == b for b in range(1, blocks + 2)]
                diff = []
                for g in range(3):
                    found = held[t, k, g]
                    for side in range(2):
                        found = jnp.where(masks[blocks - 1 + side], lane_gather(edges[g][side], lanes), found)
                    diff.append(found - here[g])
                diff.append(pick(pressures, lanes, masks) - here[3])
                east, north, smooth = east_of[t, k], north_of[t, k], smooth_of[t, k]
                lap0 = lap0 + smooth * diff[0]
                lap1 = lap1 + smooth * diff[1]
                lap2 = lap2 + smooth * diff[2]
                east2 = east2 + east * diff[2]
                north2 = north2 + north * diff[2]
                east3 = east3 + east * diff[3]
                north3 = north3 + north * diff[3]
            bottom = wide(bot[pl.ds(t, 1), :])
            turn = wide(cor[pl.ds(t, 1), :])
            drag = jnp.where(level_ids == bottom - 1, drag_rate, 0.0)
            u, v, rho = here[:3]
            push0 = -east3 + turn * v + lap0 - drag * u
            push1 = -north3 - turn * u + lap1 - drag * v
            wet = level_ids < bottom
            own[0, t] = jnp.where(wet, u + time_step * push0, 0.0)
            own[1, t] = jnp.where(wet, v + time_step * push1, 0.0)
            own[2, t] = rho + time_step * (lap2 - u * east2 - v * north2)
            return 0
        lax.fori_loop(0, blocks, body, 0)

    expected = (n_space - 1) + (n_level - 1) * (1 + low + high)
    pl.semaphore_wait(barrier, expected)

    def step(s, _):
        make_small(s)
        send_out(s)
        gather_own()
        receive(s)
        columns(s)
        surface(s)

        @pl.when(s == STEPS - 1)
        def _():
            def start(d, _):
                vol_copy(lax.rem(sp + d, n_space), sp).start()
                return 0
            lax.fori_loop(1, n_space, start, 0)

        advance(s)
        close(s)
        return 0

    lax.fori_loop(0, STEPS, step, 0)

    for t in range(blocks):
        here = slice(t * LANES, (t + 1) * LANES)
        vel_out[0, :, here] = own[0, t]
        vel_out[1, :, here] = own[1, t]
        den_out[:, here] = own[2, t]

    def collect(d, total):
        q = lax.rem(sp + d, n_space)
        vol_copy(q, q).wait_recv()
        return total + vol_all[q]

    total = lax.fori_loop(1, n_space, collect, vol[...])
    sums = jnp.sum(total, axis=1, keepdims=True)
    drifts = sums / sums[STEPS:STEPS + 1]
    shift = jnp.sum(drifts[:STEPS], axis=0, keepdims=True)
    for t in range(blocks):
        ele_out[t:t + 1, :] = eta[t][:1] + time_step * shift
    drift_out[...] = jnp.broadcast_to(drifts, (8, LANES))

    def finish(d, _):
        vol_copy(lax.rem(sp + d, n_space), sp).wait_send()
        return 0

    lax.fori_loop(1, n_space, finish, 0)


def solution(mesh):
    n_space, n_level = mesh.shape["space"], mesh.shape["level"]

    def local(velocity, density, elevation, grad_weights, lap_weights, coriolis,
              node_area, thickness, send_list, neighbours, bottom):
        rows, nodes = density.shape
        blocks = nodes // LANES
        near_count = neighbours.shape[0]
        f32, i32 = jnp.float32, jnp.int32
        plane = (blocks, LANES)
        vmem = pl.BlockSpec(memory_space=pltpu.VMEM)
        smem = pl.BlockSpec(memory_space=pltpu.SMEM)
        dma = pltpu.SemaphoreType.DMA
        tile = (rows, LANES)
        out = pl.pallas_call(
            functools.partial(kernel, n_space, n_level, rows, blocks, near_count),
            out_shape=(
                jax.ShapeDtypeStruct(velocity.shape, f32),
                jax.ShapeDtypeStruct(density.shape, f32),
                jax.ShapeDtypeStruct(plane, f32),
                jax.ShapeDtypeStruct((8, LANES), f32),
            ),
            in_specs=[vmem] * 7 + [smem] + [vmem] * 3,
            out_specs=(vmem,) * 4,
            scratch_shapes=[
                pltpu.VMEM((3, blocks) + tile, f32),
                pltpu.VMEM((blocks, 8, LANES), f32),
                pltpu.VMEM((blocks, near_count) + tile, i32),
                pltpu.VMEM((blocks, near_count) + tile, i32),
                pltpu.VMEM((blocks, near_count) + tile, f32),
                pltpu.VMEM((blocks, near_count) + tile, f32),
                pltpu.VMEM((blocks, near_count) + tile, f32),
                pltpu.VMEM((blocks, near_count, 8, LANES), f32),
                pltpu.VMEM((blocks, near_count, 3) + tile, f32),
                pltpu.VMEM((blocks + 2,) + tile, f32),
                pltpu.VMEM((blocks + 2, 8, LANES), f32),
                pltpu.VMEM((STEPS, blocks, 8, LANES), f32),
                pltpu.VMEM((STEPS, 2, 3 * rows + 8, LANES), f32),
                pltpu.VMEM((STEPS, 2, 3 * rows + 8, LANES), f32),
                pltpu.VMEM((STEPS, 2, n_level, 8, LANES), f32),
                pltpu.VMEM((STEPS, n_level, blocks, 8, LANES), f32),
                pltpu.VMEM((8, LANES), f32),
                pltpu.VMEM((n_space, 8, LANES), f32),
                dma((STEPS, 2)), dma((STEPS, 2)),
                dma((STEPS, 2, n_level)), dma((STEPS, 2, n_level)),
                dma((STEPS, n_level)), dma((STEPS, n_level)),
                dma((n_space,)), dma((n_space,)),
            ],
            compiler_params=pltpu.CompilerParams(collective_id=0, has_side_effects=True),
        )(velocity, density, elevation.reshape(plane), grad_weights, lap_weights,
          coriolis.reshape(plane), node_area.reshape(plane), thickness, send_list,
          neighbours, bottom.reshape(plane))
        return out[0], out[1], out[2].reshape(nodes), out[3][:STEPS, 0]

    return jax.shard_map(
        local,
        mesh=mesh,
        in_specs=(
            P(None, "level", "space"),
            P("level", "space"),
            P("space"),
            P(None, None, "space"),
            P(None, "space"),
            P("space"),
            P("space"),
            P("level"),
            P("space", None),
            P(None, "space"),
            P("space"),
        ),
        out_specs=(P(None, "level", "space"), P("level", "space"), P("space"), P()),
        check_vma=False,
    )
```

```python
import functools

import jax
import jax.numpy as jnp
from jax import lax
from jax.experimental import pallas as pl
from jax.experimental.pallas import tpu as pltpu
from jax.sharding import PartitionSpec as P

STEPS = 4
LANES = 128

time_step = 0.1
buoyancy = 0.5
drag_rate = 0.5


def lane_gather(values, lanes):
    return jnp.take_along_axis(values, lanes, axis=1, mode="promise_in_bounds")


def pick(tiles, lanes, masks):
    found = lane_gather(tiles[0], lanes)
    for tile, mask in zip(tiles[1:], masks):
        found = jnp.where(mask, lane_gather(tile, lanes), found)
    return found


def running_sum(values, rows, row_ids):
    shift = 1
    while shift < rows:
        moved = pltpu.roll(values, shift, 0)
        values = values + jnp.where(row_ids >= shift, moved, 0.0)
        shift *= 2
    return values


def kernel(
    n_space, n_level, rows, blocks, near_count,
    vel, den, ele, grad, lap, cor, area, thick, send, near, bot,
    vel_out, den_out, ele_out, drift_out,
    own, eta, lanes_of, block_of, east_of, north_of, smooth_of,
    flow_lanes, flow_block, flow_of, held, flow_held, press, flow, small, out, halo, halo_small, peer,
    vol, vol_all,
    main_send, main_recv, hs_send, hs_recv, peer_send, peer_recv, vol_send, vol_recv,
):
    sp = lax.axis_index("space")
    lv = lax.axis_index("level")
    has = (sp > 0, sp < n_space - 1)
    ends = (sp - 1, sp + 1)

    barrier = pltpu.get_barrier_semaphore()

    def greet(d, _):
        pl.semaphore_signal(barrier, inc=1, device_id={"space": lax.rem(sp + d, n_space), "level": lv})
        return 0

    lax.fori_loop(1, n_space, greet, 0)
    for d in range(1, n_level):
        q = lax.rem(lv + d, n_level)
        pl.semaphore_signal(barrier, inc=1, device_id={"space": sp, "level": q})
        for side in range(2):
            @pl.when(has[side])
            def _():
                pl.semaphore_signal(barrier, inc=1, device_id={"space": ends[side], "level": q})

    row_ids = lax.broadcasted_iota(jnp.int32, (rows, LANES), 0)
    eight = lax.broadcasted_iota(jnp.int32, (8, LANES), 0)
    odd = jnp.bitwise_and(eight, 1) == 1
    level_ids = row_ids + lv * rows
    thickness = jnp.zeros((rows, LANES), jnp.float32)
    for r in range(rows):
        thickness = jnp.where(row_ids == r, thick[r], thickness)

    def wide(row, count=rows):
        return jnp.broadcast_to(row, (count, LANES))

    low = jnp.where(has[0], 1, 0)
    high = jnp.where(has[1], 1, 0)

    def prepare(t, _):
        here = pl.ds(pl.multiple_of(t * LANES, LANES), LANES)
        bottom = wide(bot[pl.ds(t, 1), :])
        wet = level_ids < bottom
        own[0, t] = jnp.where(wet, vel[0, :, here], 0.0)
        own[1, t] = jnp.where(wet, vel[1, :, here], 0.0)
        own[2, t] = den[:, here]
        eta[t] = wide(ele[pl.ds(t, 1), :], 8)
        for k in range(near_count):
            slot = wide(near[k:k + 1, here])
            block = lax.shift_right_logical(slot, 7)
            inside = jnp.where(block < blocks, 1, jnp.where(block == blocks, low, high))
            valid = inside > 0
            lanes_of[t, k] = jnp.bitwise_and(slot, LANES - 1)
            block_of[t, k] = jnp.where(valid, block, 0)
            east = jnp.where(valid, wide(grad[k, 0:1, here]), 0.0)
            north = jnp.where(valid, wide(grad[k, 1:2, here]), 0.0)
            east_of[t, k] = east
            north_of[t, k] = north
            smooth_of[t, k] = jnp.where(valid, wide(lap[k:k + 1, here]), 0.0)
        for j in range(flow_of.shape[1]):
            lane_pack = jnp.zeros((8, LANES), jnp.int32)
            block_pack = jnp.zeros((8, LANES), jnp.int32)
            pack = jnp.zeros((8, LANES), jnp.float32)
            for k in range(4 * j, min(4 * j + 4, near_count)):
                first = 2 * (k - 4 * j)
                mine = jnp.logical_or(eight == first, eight == first + 1)
                lane_pack = jnp.where(mine, lanes_of[t, k, :8], lane_pack)
                block_pack = jnp.where(mine, block_of[t, k, :8], block_pack)
                pack = jnp.where(eight == first, east_of[t, k, :8], pack)
                pack = jnp.where(eight == first + 1, north_of[t, k, :8], pack)
            flow_lanes[t, j] = lane_pack
            flow_block[t, j] = block_pack
            flow_of[t, j] = pack
        return 0

    lax.fori_loop(0, blocks, prepare, 0)
    wet_area = area[...] * jnp.where(bot[...] > 0, 1.0, 0.0)
    vol[...] = jnp.where(eight == STEPS, wide(jnp.sum(wet_area, axis=0, keepdims=True), 8), 0.0)

    def main_copy(s, side):
        return pltpu.make_async_remote_copy(
            src_ref=out.at[s, side], dst_ref=halo.at[s, 1 - side],
            send_sem=main_send.at[s, side], recv_sem=main_recv.at[s, 1 - side],
            device_id={"space": ends[side], "level": lv}, device_id_type=pl.DeviceIdType.MESH)

    def small_copy(s, side, q, slot):
        return pltpu.make_async_remote_copy(
            src_ref=out.at[s, side, pl.ds(3 * rows, 8)], dst_ref=halo_small.at[s, 1 - side, slot],
            send_sem=hs_send.at[s, side, q], recv_sem=hs_recv.at[s, 1 - side, slot],
            device_id={"space": ends[side], "level": q}, device_id_type=pl.DeviceIdType.MESH)

    def peer_copy(s, q, slot):
        return pltpu.make_async_remote_copy(
            src_ref=small.at[s], dst_ref=peer.at[s, slot],
            send_sem=peer_send.at[s, q], recv_sem=peer_recv.at[s, slot],
            device_id={"space": sp, "level": q}, device_id_type=pl.DeviceIdType.MESH)

    def vol_copy(q, slot):
        return pltpu.make_async_remote_copy(
            src_ref=vol, dst_ref=vol_all.at[slot],
            send_sem=vol_send.at[q], recv_sem=vol_recv.at[slot],
            device_id={"space": q, "level": lv}, device_id_type=pl.DeviceIdType.MESH)

    others = [lax.rem(lv + d, n_level) for d in range(1, n_level)]

    def make_small(s):
        def body(t, _):
            total = jnp.sum(own[2, t] * thickness, axis=0, keepdims=True)
            flow0 = jnp.sum(own[0, t] * thickness, axis=0, keepdims=True)
            flow1 = jnp.sum(own[1, t] * thickness, axis=0, keepdims=True)
            tile = jnp.where(eight == 0, wide(flow0, 8), jnp.where(eight == 1, wide(flow1, 8), 0.0))
            tile = jnp.where(eight == 2, wide(total, 8), tile)
            small[s, t] = jnp.where(eight == 3, eta[t], tile)
            return 0
        lax.fori_loop(0, blocks, body, 0, unroll=True)

    def send_out(s):
        for side in range(2):
            slot = wide(send[:, side * LANES:(side + 1) * LANES])
            lanes = jnp.bitwise_and(slot, LANES - 1)
            block = lax.shift_right_logical(slot, 7)
            masks = [block == b for b in range(1, blocks)]
            for g in range(3):
                out[s, side, g * rows:(g + 1) * rows] = pick([own[g, b] for b in range(blocks)], lanes, masks)
            out[s, side, 3 * rows:3 * rows + 8] = pick(
                [small[s, b] for b in range(blocks)], lanes[:8], [m[:8] for m in masks])
        for q in others:
            peer_copy(s, q, lv).start()
        for side in range(2):
            @pl.when(has[side])
            def _():
                for q in others:
                    small_copy(s, side, q, lv).start()
                main_copy(s, side).start()

    def gather_own():
        def body(t, _):
            tiles = [[own[g, b] for b in range(blocks)] for g in range(3)]
            for k in range(near_count):
                lanes = lanes_of[t, k]
                block = block_of[t, k]
                masks = [block == b for b in range(1, blocks)]
                for g in range(3):
                    held[t, k, g] = pick(tiles[g], lanes, masks)
            return 0
        lax.fori_loop(0, blocks, body, 0)

    def receive(s):
        for side in range(2):
            @pl.when(has[side])
            def _():
                main_copy(s, 1 - side).wait_recv()
                for q in others:
                    small_copy(s, 1 - side, q, q).wait_recv()

    def close(s):
        for q in others:
            peer_copy(s, q, lv).wait_send()
        for side in range(2):
            @pl.when(has[side])
            def _():
                main_copy(s, side).wait_send()
                for q in others:
                    small_copy(s, side, q, lv).wait_send()

    def finish_column(slot, density, mine, pieces):
        above = jnp.zeros((1, LANES), jnp.float32)
        total = mine
        for q, piece in zip(others, pieces):
            total = total + piece
            above = above + jnp.where(q < lv, piece[2:3], 0.0)
        weighted = density * thickness
        column = wide(above) + running_sum(weighted, rows, row_ids) - 0.5 * weighted
        press[slot] = wide(mine[3:4]) + buoyancy * column
        flow[slot] = jnp.where(odd, wide(total[1:2], 8), wide(total[0:1], 8))

    def own_columns(s):
        def body(t, _):
            finish_column(t, own[2, t], small[s, t], [peer[s, q, t] for q in others])
            return 0
        lax.fori_loop(0, blocks, body, 0, unroll=True)

    def halo_columns(s):
        for side in range(2):
            finish_column(blocks + side, halo[s, side, 2 * rows:3 * rows], halo[s, side, 3 * rows:3 * rows + 8],
                          [halo_small[s, side, q] for q in others])

    def gather_columns():
        pressures = [press[b] for b in range(blocks)]
        flows = [flow[b] for b in range(blocks)]

        def body(t, _):
            for k in range(near_count):
                block = block_of[t, k]
                held[t, k, 3] = pick(pressures, lanes_of[t, k], [block == b for b in range(1, blocks)])
            for j in range(flow_of.shape[1]):
                block = flow_block[t, j]
                flow_held[t, j] = pick(flows, flow_lanes[t, j], [block == b for b in range(1, blocks)])
            return 0
        lax.fori_loop(0, blocks, body, 0)

    def surface(s):
        sides = [flow[blocks], flow[blocks + 1]]

        def body(t, volume):
            middle = flow[t]
            total = jnp.zeros((8, LANES), jnp.float32)
            for j in range(flow_of.shape[1]):
                lanes, block, found = flow_lanes[t, j], flow_block[t, j], flow_held[t, j]
                for side in range(2):
                    found = jnp.where(block == blocks + side, lane_gather(sides[side], lanes), found)
                total = total + flow_of[t, j] * (found - middle)
            diverge = jnp.sum(total, axis=0, keepdims=True)
            wet_node = jnp.where(bot[pl.ds(t, 1), :] > 0, 1.0, 0.0)
            part = wet_node * diverge
            eta[t] = eta[t] - time_step * wide(part, 8)
            return volume + area[pl.ds(t, 1), :] * part

        volume = lax.fori_loop(0, blocks, body, jnp.zeros((1, LANES), jnp.float32), unroll=True)
        vol[...] = jnp.where(eight == s, wide(volume, 8), vol[...])

    def advance(s):
        edges = [[halo[s, side, g * rows:(g + 1) * rows] for side in range(2)] for g in range(3)]
        edges.append([press[blocks], press[blocks + 1]])

        def body(t, _):
            here = [own[0, t], own[1, t], own[2, t], press[t]]
            zero = jnp.zeros((rows, LANES), jnp.float32)
            lap0 = lap1 = lap2 = east2 = north2 = east3 = north3 = zero
            for k in range(near_count):
                lanes = lanes_of[t, k]
                block = block_of[t, k]
                masks = [block == blocks, block == blocks + 1]
                diff = []
                for g in range(4):
                    found = held[t, k, g]
                    for side in range(2):
                        found = jnp.where(masks[side], lane_gather(edges[g][side], lanes), found)
                    diff.append(found - here[g])
                east, north, smooth = east_of[t, k], north_of[t, k], smooth_of[t, k]
                lap0 = lap0 + smooth * diff[0]
                lap1 = lap1 + smooth * diff[1]
                lap2 = lap2 + smooth * diff[2]
                east2 = east2 + east * diff[2]
                north2 = north2 + north * diff[2]
                east3 = east3 + east * diff[3]
                north3 = north3 + north * diff[3]
            bottom = wide(bot[pl.ds(t, 1), :])
            turn = wide(cor[pl.ds(t, 1), :])
            drag = jnp.where(level_ids == bottom - 1, drag_rate, 0.0)
            u, v, rho = here[:3]
            push0 = -east3 + turn * v + lap0 - drag * u
            push1 = -north3 - turn * u + lap1 - drag * v
            wet = level_ids < bottom
            own[0, t] = jnp.where(wet, u + time_step * push0, 0.0)
            own[1, t] = jnp.where(wet, v + time_step * push1, 0.0)
            own[2, t] = rho + time_step * (lap2 - u * east2 - v * north2)
            return 0
        lax.fori_loop(0, blocks, body, 0)

    expected = (n_space - 1) + (n_level - 1) * (1 + low + high)
    pl.semaphore_wait(barrier, expected)

    def step(s, _):
        make_small(s)
        send_out(s)
        gather_own()
        for q in others:
            peer_copy(s, q, q).wait_recv()
        own_columns(s)
        gather_columns()
        receive(s)
        halo_columns(s)
        surface(s)

        @pl.when(s == STEPS - 1)
        def _():
            def start(d, _):
                vol_copy(lax.rem(sp + d, n_space), sp).start()
                return 0
            lax.fori_loop(1, n_space, start, 0)

        advance(s)
        close(s)
        return 0

    lax.fori_loop(0, STEPS, step, 0)

    for t in range(blocks):
        here = slice(t * LANES, (t + 1) * LANES)
        vel_out[0, :, here] = own[0, t]
        vel_out[1, :, here] = own[1, t]
        den_out[:, here] = own[2, t]

    def collect(d, total):
        q = lax.rem(sp + d, n_space)
        vol_copy(q, q).wait_recv()
        return total + vol_all[q]

    total = lax.fori_loop(1, n_space, collect, vol[...])
    sums = jnp.sum(total, axis=1, keepdims=True)
    drifts = sums / sums[STEPS:STEPS + 1]
    shift = jnp.sum(drifts[:STEPS], axis=0, keepdims=True)
    for t in range(blocks):
        ele_out[t:t + 1, :] = eta[t][:1] + time_step * shift
    drift_out[...] = jnp.broadcast_to(drifts, (8, LANES))

    def finish(d, _):
        vol_copy(lax.rem(sp + d, n_space), sp).wait_send()
        return 0

    lax.fori_loop(1, n_space, finish, 0)


def solution(mesh):
    n_space, n_level = mesh.shape["space"], mesh.shape["level"]

    def local(velocity, density, elevation, grad_weights, lap_weights, coriolis,
              node_area, thickness, send_list, neighbours, bottom):
        rows, nodes = density.shape
        blocks = nodes // LANES
        near_count = neighbours.shape[0]
        packs = -(-near_count // 4)
        f32, i32 = jnp.float32, jnp.int32
        plane = (blocks, LANES)
        vmem = pl.BlockSpec(memory_space=pltpu.VMEM)
        smem = pl.BlockSpec(memory_space=pltpu.SMEM)
        dma = pltpu.SemaphoreType.DMA
        tile = (rows, LANES)
        out = pl.pallas_call(
            functools.partial(kernel, n_space, n_level, rows, blocks, near_count),
            out_shape=(
                jax.ShapeDtypeStruct(velocity.shape, f32),
                jax.ShapeDtypeStruct(density.shape, f32),
                jax.ShapeDtypeStruct(plane, f32),
                jax.ShapeDtypeStruct((8, LANES), f32),
            ),
            in_specs=[vmem] * 7 + [smem] + [vmem] * 3,
            out_specs=(vmem,) * 4,
            scratch_shapes=[
                pltpu.VMEM((3, blocks) + tile, f32),
                pltpu.VMEM((blocks, 8, LANES), f32),
                pltpu.VMEM((blocks, near_count) + tile, i32),
                pltpu.VMEM((blocks, near_count) + tile, i32),
                pltpu.VMEM((blocks, near_count) + tile, f32),
                pltpu.VMEM((blocks, near_count) + tile, f32),
                pltpu.VMEM((blocks, near_count) + tile, f32),
                pltpu.VMEM((blocks, packs, 8, LANES), i32),
                pltpu.VMEM((blocks, packs, 8, LANES), i32),
                pltpu.VMEM((blocks, packs, 8, LANES), f32),
                pltpu.VMEM((blocks, near_count, 4) + tile, f32),
                pltpu.VMEM((blocks, packs, 8, LANES), f32),
                pltpu.VMEM((blocks + 2,) + tile, f32),
                pltpu.VMEM((blocks + 2, 8, LANES), f32),
                pltpu.VMEM((STEPS, blocks, 8, LANES), f32),
                pltpu.VMEM((STEPS, 2, 3 * rows + 8, LANES), f32),
                pltpu.VMEM((STEPS, 2, 3 * rows + 8, LANES), f32),
                pltpu.VMEM((STEPS, 2, n_level, 8, LANES), f32),
                pltpu.VMEM((STEPS, n_level, blocks, 8, LANES), f32),
                pltpu.VMEM((8, LANES), f32),
                pltpu.VMEM((n_space, 8, LANES), f32),
                dma((STEPS, 2)), dma((STEPS, 2)),
                dma((STEPS, 2, n_level)), dma((STEPS, 2, n_level)),
                dma((STEPS, n_level)), dma((STEPS, n_level)),
                dma((n_space,)), dma((n_space,)),
            ],
            compiler_params=pltpu.CompilerParams(collective_id=0, has_side_effects=True),
        )(velocity, density, elevation.reshape(plane), grad_weights.transpose(1, 0, 2), lap_weights,
          coriolis.reshape(plane), node_area.reshape(plane), thickness, send_list,
          neighbours, bottom.reshape(plane))
        return out[0], out[1], out[2].reshape(nodes), out[3][:STEPS, 0]

    return jax.shard_map(
        local,
        mesh=mesh,
        in_specs=(
            P(None, "level", "space"),
            P("level", "space"),
            P("space"),
            P(None, None, "space"),
            P(None, "space"),
            P("space"),
            P("space"),
            P("level"),
            P("space", None),
            P(None, "space"),
            P("space"),
        ),
        out_specs=(P(None, "level", "space"), P("level", "space"), P("space"), P()),
        check_vma=False,
    )
```

```python
import functools

import jax
import jax.numpy as jnp
from jax import lax
from jax.experimental import pallas as pl
from jax.experimental.pallas import tpu as pltpu
from jax.sharding import PartitionSpec as P

STEPS = 4
LANES = 128

time_step = 0.1
buoyancy = 0.5
drag_rate = 0.5


def lane_gather(values, lanes):
    return jnp.take_along_axis(values, lanes, axis=1, mode="promise_in_bounds")


def pick(tiles, lanes, masks):
    found = lane_gather(tiles[0], lanes)
    for tile, mask in zip(tiles[1:], masks):
        found = jnp.where(mask, lane_gather(tile, lanes), found)
    return found


def running_sum(values, rows, row_ids):
    shift = 1
    while shift < rows:
        moved = pltpu.roll(values, shift, 0)
        values = values + jnp.where(row_ids >= shift, moved, 0.0)
        shift *= 2
    return values


def kernel(
    n_space, n_level, width, rows, blocks, near_count,
    vel, den, ele, grad, lap, cor, area, thick, send, near, bot,
    vel_out, den_out, ele_out, drift_out,
    own, eta, lanes_of, block_of, east_of, north_of, smooth_of,
    flow_lanes, flow_block, flow_of, held, flow_held, press, flow, small, out, halo, halo_small, peer,
    vol, vol_all,
    main_send, main_recv, hs_send, hs_recv, peer_send, peer_recv, vol_send, vol_recv, column_in,
):
    sp = lax.axis_index("space")
    lv = lax.axis_index("level")
    has = (sp > 0, sp < n_space - 1)
    ends = (sp - 1, sp + 1)

    barrier = pltpu.get_barrier_semaphore()

    mine, place = sp // width, lax.rem(sp, width)
    column = [lax.rem(sp + d * width, n_space) for d in range(1, n_space // width)]
    row = [mine * width + lax.rem(place + d, width) for d in range(1, width)]
    for q in row + column:
        pl.semaphore_signal(barrier, inc=1, device_id={"space": q, "level": lv})
    for side in range(2):
        @pl.when(has[side])
        def _():
            pl.semaphore_signal(barrier, inc=1, device_id={"space": ends[side], "level": lv})
    for d in range(1, n_level):
        q = lax.rem(lv + d, n_level)
        pl.semaphore_signal(barrier, inc=1, device_id={"space": sp, "level": q})
        for side in range(2):
            @pl.when(has[side])
            def _():
                pl.semaphore_signal(barrier, inc=1, device_id={"space": ends[side], "level": q})

    row_ids = lax.broadcasted_iota(jnp.int32, (rows, LANES), 0)
    eight = lax.broadcasted_iota(jnp.int32, (8, LANES), 0)
    odd = jnp.bitwise_and(eight, 1) == 1
    level_ids = row_ids + lv * rows
    thickness = jnp.zeros((rows, LANES), jnp.float32)
    for r in range(rows):
        thickness = jnp.where(row_ids == r, thick[r], thickness)

    def wide(row, count=rows):
        return jnp.broadcast_to(row, (count, LANES))

    low = jnp.where(has[0], 1, 0)
    high = jnp.where(has[1], 1, 0)

    def prepare(t, _):
        here = pl.ds(pl.multiple_of(t * LANES, LANES), LANES)
        bottom = wide(bot[pl.ds(t, 1), :])
        wet = level_ids < bottom
        own[0, t] = jnp.where(wet, vel[0, :, here], 0.0)
        own[1, t] = jnp.where(wet, vel[1, :, here], 0.0)
        own[2, t] = den[:, here]
        eta[t] = wide(ele[pl.ds(t, 1), :], 8)
        for k in range(near_count):
            slot = wide(near[k:k + 1, here])
            block = lax.shift_right_logical(slot, 7)
            inside = jnp.where(block < blocks, 1, jnp.where(block == blocks, low, high))
            valid = inside > 0
            lanes_of[t, k] = jnp.bitwise_and(slot, LANES - 1)
            block_of[t, k] = jnp.where(valid, block, 0)
            east = jnp.where(valid, wide(grad[k, 0:1, here]), 0.0)
            north = jnp.where(valid, wide(grad[k, 1:2, here]), 0.0)
            east_of[t, k] = east
            north_of[t, k] = north
            smooth_of[t, k] = jnp.where(valid, wide(lap[k:k + 1, here]), 0.0)
        for j in range(flow_of.shape[1]):
            lane_pack = jnp.zeros((8, LANES), jnp.int32)
            block_pack = jnp.zeros((8, LANES), jnp.int32)
            pack = jnp.zeros((8, LANES), jnp.float32)
            for k in range(4 * j, min(4 * j + 4, near_count)):
                first = 2 * (k - 4 * j)
                mine = jnp.logical_or(eight == first, eight == first + 1)
                lane_pack = jnp.where(mine, lanes_of[t, k, :8], lane_pack)
                block_pack = jnp.where(mine, block_of[t, k, :8], block_pack)
                pack = jnp.where(eight == first, east_of[t, k, :8], pack)
                pack = jnp.where(eight == first + 1, north_of[t, k, :8], pack)
            flow_lanes[t, j] = lane_pack
            flow_block[t, j] = block_pack
            flow_of[t, j] = pack
        return 0

    lax.fori_loop(0, blocks, prepare, 0)
    wet_area = area[...] * jnp.where(bot[...] > 0, 1.0, 0.0)
    vol[...] = jnp.where(eight == STEPS, wide(jnp.sum(wet_area, axis=0, keepdims=True), 8), 0.0)

    def main_copy(s, side):
        return pltpu.make_async_remote_copy(
            src_ref=out.at[s, side], dst_ref=halo.at[s, 1 - side],
            send_sem=main_send.at[s, side], recv_sem=main_recv.at[s, 1 - side],
            device_id={"space": ends[side], "level": lv}, device_id_type=pl.DeviceIdType.MESH)

    def small_copy(s, side, q, slot):
        return pltpu.make_async_remote_copy(
            src_ref=out.at[s, side, pl.ds(3 * rows, 8)], dst_ref=halo_small.at[s, 1 - side, slot],
            send_sem=hs_send.at[s, side, q], recv_sem=hs_recv.at[s, 1 - side, slot],
            device_id={"space": ends[side], "level": q}, device_id_type=pl.DeviceIdType.MESH)

    def peer_copy(s, q, slot):
        return pltpu.make_async_remote_copy(
            src_ref=small.at[s], dst_ref=peer.at[s, slot],
            send_sem=peer_send.at[s, q], recv_sem=peer_recv.at[s, slot],
            device_id={"space": sp, "level": q}, device_id_type=pl.DeviceIdType.MESH)

    def vol_copy(q, slot):
        return pltpu.make_async_remote_copy(
            src_ref=vol, dst_ref=vol_all.at[slot],
            send_sem=vol_send.at[q], recv_sem=vol_recv.at[slot],
            device_id={"space": q, "level": lv}, device_id_type=pl.DeviceIdType.MESH)

    others = [lax.rem(lv + d, n_level) for d in range(1, n_level)]

    def make_small(s):
        def body(t, _):
            total = jnp.sum(own[2, t] * thickness, axis=0, keepdims=True)
            flow0 = jnp.sum(own[0, t] * thickness, axis=0, keepdims=True)
            flow1 = jnp.sum(own[1, t] * thickness, axis=0, keepdims=True)
            tile = jnp.where(eight == 0, wide(flow0, 8), jnp.where(eight == 1, wide(flow1, 8), 0.0))
            tile = jnp.where(eight == 2, wide(total, 8), tile)
            small[s, t] = jnp.where(eight == 3, eta[t], tile)
            return 0
        lax.fori_loop(0, blocks, body, 0, unroll=True)

    def send_out(s):
        for side in range(2):
            slot = wide(send[:, side * LANES:(side + 1) * LANES])
            lanes = jnp.bitwise_and(slot, LANES - 1)
            block = lax.shift_right_logical(slot, 7)
            masks = [block == b for b in range(1, blocks)]
            for g in range(3):
                out[s, side, g * rows:(g + 1) * rows] = pick([own[g, b] for b in range(blocks)], lanes, masks)
            out[s, side, 3 * rows:3 * rows + 8] = pick(
                [small[s, b] for b in range(blocks)], lanes[:8], [m[:8] for m in masks])
        for q in others:
            peer_copy(s, q, lv).start()
        for side in range(2):
            @pl.when(has[side])
            def _():
                for q in others:
                    small_copy(s, side, q, lv).start()
                main_copy(s, side).start()

    def gather_own():
        def body(t, _):
            tiles = [[own[g, b] for b in range(blocks)] for g in range(3)]
            for k in range(near_count):
                lanes = lanes_of[t, k]
                block = block_of[t, k]
                masks = [block == b for b in range(1, blocks)]
                for g in range(3):
                    held[t, k, g] = pick(tiles[g], lanes, masks)
            return 0
        lax.fori_loop(0, blocks, body, 0)

    def receive(s):
        for side in range(2):
            @pl.when(has[side])
            def _():
                main_copy(s, 1 - side).wait_recv()
                for q in others:
                    small_copy(s, 1 - side, q, q).wait_recv()

    def close(s):
        for q in others:
            peer_copy(s, q, lv).wait_send()
        for side in range(2):
            @pl.when(has[side])
            def _():
                main_copy(s, side).wait_send()
                for q in others:
                    small_copy(s, side, q, lv).wait_send()

    def finish_column(slot, density, mine, pieces):
        above = jnp.zeros((1, LANES), jnp.float32)
        total = mine
        for q, piece in zip(others, pieces):
            total = total + piece
            above = above + jnp.where(q < lv, piece[2:3], 0.0)
        weighted = density * thickness
        column = wide(above) + running_sum(weighted, rows, row_ids) - 0.5 * weighted
        press[slot] = wide(mine[3:4]) + buoyancy * column
        flow[slot] = jnp.where(odd, wide(total[1:2], 8), wide(total[0:1], 8))

    def own_columns(s):
        def body(t, _):
            finish_column(t, own[2, t], small[s, t], [peer[s, q, t] for q in others])
            return 0
        lax.fori_loop(0, blocks, body, 0, unroll=True)

    def halo_columns(s):
        for side in range(2):
            finish_column(blocks + side, halo[s, side, 2 * rows:3 * rows], halo[s, side, 3 * rows:3 * rows + 8],
                          [halo_small[s, side, q] for q in others])

    def gather_columns():
        pressures = [press[b] for b in range(blocks)]
        flows = [flow[b] for b in range(blocks)]

        def body(t, _):
            for k in range(near_count):
                block = block_of[t, k]
                held[t, k, 3] = pick(pressures, lanes_of[t, k], [block == b for b in range(1, blocks)])
            for j in range(flow_of.shape[1]):
                block = flow_block[t, j]
                flow_held[t, j] = pick(flows, flow_lanes[t, j], [block == b for b in range(1, blocks)])
            return 0
        lax.fori_loop(0, blocks, body, 0)

    def surface(s):
        sides = [flow[blocks], flow[blocks + 1]]

        def body(t, volume):
            middle = flow[t]
            total = jnp.zeros((8, LANES), jnp.float32)
            for j in range(flow_of.shape[1]):
                lanes, block, found = flow_lanes[t, j], flow_block[t, j], flow_held[t, j]
                for side in range(2):
                    found = jnp.where(block == blocks + side, lane_gather(sides[side], lanes), found)
                total = total + flow_of[t, j] * (found - middle)
            diverge = jnp.sum(total, axis=0, keepdims=True)
            wet_node = jnp.where(bot[pl.ds(t, 1), :] > 0, 1.0, 0.0)
            part = wet_node * diverge
            eta[t] = eta[t] - time_step * wide(part, 8)
            return volume + area[pl.ds(t, 1), :] * part

        volume = lax.fori_loop(0, blocks, body, jnp.zeros((1, LANES), jnp.float32), unroll=True)
        vol[...] = jnp.where(eight == s, wide(volume, 8), vol[...])

    def advance(s):
        edges = [[halo[s, side, g * rows:(g + 1) * rows] for side in range(2)] for g in range(3)]
        edges.append([press[blocks], press[blocks + 1]])

        def body(t, _):
            here = [own[0, t], own[1, t], own[2, t], press[t]]
            zero = jnp.zeros((rows, LANES), jnp.float32)
            lap0 = lap1 = lap2 = east2 = north2 = east3 = north3 = zero
            for k in range(near_count):
                lanes = lanes_of[t, k]
                block = block_of[t, k]
                masks = [block == blocks, block == blocks + 1]
                diff = []
                for g in range(4):
                    found = held[t, k, g]
                    for side in range(2):
                        found = jnp.where(masks[side], lane_gather(edges[g][side], lanes), found)
                    diff.append(found - here[g])
                east, north, smooth = east_of[t, k], north_of[t, k], smooth_of[t, k]
                lap0 = lap0 + smooth * diff[0]
                lap1 = lap1 + smooth * diff[1]
                lap2 = lap2 + smooth * diff[2]
                east2 = east2 + east * diff[2]
                north2 = north2 + north * diff[2]
                east3 = east3 + east * diff[3]
                north3 = north3 + north * diff[3]
            bottom = wide(bot[pl.ds(t, 1), :])
            turn = wide(cor[pl.ds(t, 1), :])
            drag = jnp.where(level_ids == bottom - 1, drag_rate, 0.0)
            u, v, rho = here[:3]
            push0 = -east3 + turn * v + lap0 - drag * u
            push1 = -north3 - turn * u + lap1 - drag * v
            wet = level_ids < bottom
            own[0, t] = jnp.where(wet, u + time_step * push0, 0.0)
            own[1, t] = jnp.where(wet, v + time_step * push1, 0.0)
            own[2, t] = rho + time_step * (lap2 - u * east2 - v * north2)
            return 0
        lax.fori_loop(0, blocks, body, 0)

    expected = len(row) + len(column) + low + high + (n_level - 1) * (1 + low + high)
    pl.semaphore_wait(barrier, expected)
    for q in row:
        pl.semaphore_signal(column_in, inc=1, device_id={"space": q, "level": lv})

    def step(s, _):
        make_small(s)
        send_out(s)
        gather_own()
        for q in others:
            peer_copy(s, q, q).wait_recv()
        own_columns(s)
        gather_columns()
        receive(s)
        halo_columns(s)
        surface(s)

        @pl.when(s == STEPS - 1)
        def _():
            pl.semaphore_wait(column_in, len(row))

            def start(d, _):
                vol_copy(lax.rem(sp + d, n_space), sp).start()
                return 0
            lax.fori_loop(1, n_space, start, 0)

        advance(s)
        close(s)
        return 0

    lax.fori_loop(0, STEPS, step, 0)

    for t in range(blocks):
        here = slice(t * LANES, (t + 1) * LANES)
        vel_out[0, :, here] = own[0, t]
        vel_out[1, :, here] = own[1, t]
        den_out[:, here] = own[2, t]

    def collect(d, total):
        q = lax.rem(sp + d, n_space)
        vol_copy(q, q).wait_recv()
        return total + vol_all[q]

    total = lax.fori_loop(1, n_space, collect, vol[...])
    sums = jnp.sum(total, axis=1, keepdims=True)
    drifts = sums / sums[STEPS:STEPS + 1]
    shift = jnp.sum(drifts[:STEPS], axis=0, keepdims=True)
    for t in range(blocks):
        ele_out[t:t + 1, :] = eta[t][:1] + time_step * shift
    lane_ids = lax.broadcasted_iota(jnp.int32, (1, LANES), 1)
    line = jnp.zeros((1, LANES), jnp.float32)
    for s in range(STEPS):
        line = jnp.where(lane_ids == s, drifts[s:s + 1], line)
    drift_out[...] = line

    def finish(d, _):
        vol_copy(lax.rem(sp + d, n_space), sp).wait_send()
        return 0

    lax.fori_loop(1, n_space, finish, 0)


def emit(vel, den, ele, drift, vel_out, den_out, ele_out, drift_out):
    vel_out[...] = vel[...]
    den_out[...] = den[...]
    ele_out[...] = ele[...]
    drift_out[...] = drift[:, :STEPS]


def solution(mesh):
    n_space, n_level = mesh.shape["space"], mesh.shape["level"]
    width = max(w for w in range(1, n_space + 1) if n_space % w == 0 and w * w <= n_space)

    def local(velocity, density, elevation, grad_weights, lap_weights, coriolis,
              node_area, thickness, send_list, neighbours, bottom):
        rows, nodes = density.shape
        blocks = nodes // LANES
        near_count = neighbours.shape[0]
        packs = -(-near_count // 4)
        f32, i32 = jnp.float32, jnp.int32
        plane = (blocks, LANES)
        vmem = pl.BlockSpec(memory_space=pltpu.VMEM)
        smem = pl.BlockSpec(memory_space=pltpu.SMEM)
        dma = pltpu.SemaphoreType.DMA
        tile = (rows, LANES)
        out = pl.pallas_call(
            functools.partial(kernel, n_space, n_level, width, rows, blocks, near_count),
            out_shape=(
                jax.ShapeDtypeStruct(velocity.shape, f32),
                jax.ShapeDtypeStruct(density.shape, f32),
                jax.ShapeDtypeStruct(plane, f32),
                jax.ShapeDtypeStruct((1, LANES), f32),
            ),
            in_specs=[vmem] * 7 + [smem] + [vmem] * 3,
            out_specs=(vmem,) * 4,
            scratch_shapes=[
                pltpu.VMEM((3, blocks) + tile, f32),
                pltpu.VMEM((blocks, 8, LANES), f32),
                pltpu.VMEM((blocks, near_count) + tile, i32),
                pltpu.VMEM((blocks, near_count) + tile, i32),
                pltpu.VMEM((blocks, near_count) + tile, f32),
                pltpu.VMEM((blocks, near_count) + tile, f32),
                pltpu.VMEM((blocks, near_count) + tile, f32),
                pltpu.VMEM((blocks, packs, 8, LANES), i32),
                pltpu.VMEM((blocks, packs, 8, LANES), i32),
                pltpu.VMEM((blocks, packs, 8, LANES), f32),
                pltpu.VMEM((blocks, near_count, 4) + tile, f32),
                pltpu.VMEM((blocks, packs, 8, LANES), f32),
                pltpu.VMEM((blocks + 2,) + tile, f32),
                pltpu.VMEM((blocks + 2, 8, LANES), f32),
                pltpu.VMEM((STEPS, blocks, 8, LANES), f32),
                pltpu.VMEM((STEPS, 2, 3 * rows + 8, LANES), f32),
                pltpu.VMEM((STEPS, 2, 3 * rows + 8, LANES), f32),
                pltpu.VMEM((STEPS, 2, n_level, 8, LANES), f32),
                pltpu.VMEM((STEPS, n_level, blocks, 8, LANES), f32),
                pltpu.VMEM((8, LANES), f32),
                pltpu.VMEM((n_space, 8, LANES), f32),
                dma((STEPS, 2)), dma((STEPS, 2)),
                dma((STEPS, 2, n_level)), dma((STEPS, 2, n_level)),
                dma((STEPS, n_level)), dma((STEPS, n_level)),
                dma((n_space,)), dma((n_space,)),
                pltpu.SemaphoreType.REGULAR,
            ],
            compiler_params=pltpu.CompilerParams(collective_id=0, has_side_effects=True),
        )(velocity, density, elevation.reshape(plane), grad_weights.transpose(1, 0, 2), lap_weights,
          coriolis.reshape(plane), node_area.reshape(plane), thickness, send_list,
          neighbours, bottom.reshape(plane))
        out = pl.pallas_call(
            emit,
            out_shape=(
                jax.ShapeDtypeStruct(velocity.shape, f32),
                jax.ShapeDtypeStruct(density.shape, f32),
                jax.ShapeDtypeStruct(plane, f32),
                jax.ShapeDtypeStruct((1, STEPS), f32),
            ),
            in_specs=[vmem] * 4,
            out_specs=(vmem,) * 4,
        )(*out)
        return out[0], out[1], out[2].reshape(nodes), out[3].reshape(STEPS)

    return jax.shard_map(
        local,
        mesh=mesh,
        in_specs=(
            P(None, "level", "space"),
            P("level", "space"),
            P("space"),
            P(None, None, "space"),
            P(None, "space"),
            P("space"),
            P("space"),
            P("level"),
            P("space", None),
            P(None, "space"),
            P("space"),
        ),
        out_specs=(P(None, "level", "space"), P("level", "space"), P("space"), P()),
        check_vma=False,
    )
```

```python
import functools

import jax
import jax.numpy as jnp
from jax import lax
from jax.experimental import pallas as pl
from jax.experimental.pallas import tpu as pltpu
from jax.sharding import PartitionSpec as P

STEPS = 4
LANES = 128

time_step = 0.1
buoyancy = 0.5
drag_rate = 0.5


def lane_gather(values, lanes):
    return jnp.take_along_axis(values, lanes, axis=1, mode="promise_in_bounds")


def pick(tiles, lanes, masks):
    found = lane_gather(tiles[0], lanes)
    for tile, mask in zip(tiles[1:], masks):
        found = jnp.where(mask, lane_gather(tile, lanes), found)
    return found


def running_sum(values, rows, row_ids):
    shift = 1
    while shift < rows:
        moved = pltpu.roll(values, shift, 0)
        values = values + jnp.where(row_ids >= shift, moved, 0.0)
        shift *= 2
    return values


def kernel(
    n_space, n_level, width, rows, blocks, near_count,
    vel, den, ele, grad, lap, cor, area, thick, send, near, bot,
    vel_out, den_out, ele_out, drift_out,
    own, eta, lanes_of, block_of, east_of, north_of, smooth_of,
    flow_lanes, flow_block, flow_of, held, flow_held, press, flow, small, out, halo, halo_small, peer,
    vol, vol_line, vol_all,
    main_send, main_recv, hs_send, hs_recv, peer_send, peer_recv, vol_send, vol_recv, column_in,
):
    sp = lax.axis_index("space")
    lv = lax.axis_index("level")
    has = (sp > 0, sp < n_space - 1)
    ends = (sp - 1, sp + 1)

    barrier = pltpu.get_barrier_semaphore()

    mine, place = sp // width, lax.rem(sp, width)
    column = [lax.rem(sp + d * width, n_space) for d in range(1, n_space // width)]
    row = [mine * width + lax.rem(place + d, width) for d in range(1, width)]
    for q in row + column:
        pl.semaphore_signal(barrier, inc=1, device_id={"space": q, "level": lv})
    for side in range(2):
        @pl.when(has[side])
        def _():
            pl.semaphore_signal(barrier, inc=1, device_id={"space": ends[side], "level": lv})
    for d in range(1, n_level):
        q = lax.rem(lv + d, n_level)
        pl.semaphore_signal(barrier, inc=1, device_id={"space": sp, "level": q})
        for side in range(2):
            @pl.when(has[side])
            def _():
                pl.semaphore_signal(barrier, inc=1, device_id={"space": ends[side], "level": q})

    row_ids = lax.broadcasted_iota(jnp.int32, (rows, LANES), 0)
    eight = lax.broadcasted_iota(jnp.int32, (8, LANES), 0)
    odd = jnp.bitwise_and(eight, 1) == 1
    lane_ids = lax.broadcasted_iota(jnp.int32, (1, LANES), 1)
    level_ids = row_ids + lv * rows
    thickness = jnp.zeros((rows, LANES), jnp.float32)
    for r in range(rows):
        thickness = jnp.where(row_ids == r, thick[r], thickness)

    def wide(row, count=rows):
        return jnp.broadcast_to(row, (count, LANES))

    low = jnp.where(has[0], 1, 0)
    high = jnp.where(has[1], 1, 0)

    def prepare(t, _):
        here = pl.ds(pl.multiple_of(t * LANES, LANES), LANES)
        bottom = wide(bot[pl.ds(t, 1), :])
        wet = level_ids < bottom
        own[0, t] = jnp.where(wet, vel[0, :, here], 0.0)
        own[1, t] = jnp.where(wet, vel[1, :, here], 0.0)
        own[2, t] = den[:, here]
        eta[t] = wide(ele[pl.ds(t, 1), :], 8)
        for k in range(near_count):
            slot = wide(near[k:k + 1, here])
            block = lax.shift_right_logical(slot, 7)
            inside = jnp.where(block < blocks, 1, jnp.where(block == blocks, low, high))
            valid = inside > 0
            lanes_of[t, k] = jnp.bitwise_and(slot, LANES - 1)
            block_of[t, k] = jnp.where(valid, block, 0)
            east = jnp.where(valid, wide(grad[k, 0:1, here]), 0.0)
            north = jnp.where(valid, wide(grad[k, 1:2, here]), 0.0)
            east_of[t, k] = east
            north_of[t, k] = north
            smooth_of[t, k] = jnp.where(valid, wide(lap[k:k + 1, here]), 0.0)
        for j in range(flow_of.shape[1]):
            lane_pack = jnp.zeros((8, LANES), jnp.int32)
            block_pack = jnp.zeros((8, LANES), jnp.int32)
            pack = jnp.zeros((8, LANES), jnp.float32)
            for k in range(4 * j, min(4 * j + 4, near_count)):
                first = 2 * (k - 4 * j)
                mine = jnp.logical_or(eight == first, eight == first + 1)
                lane_pack = jnp.where(mine, lanes_of[t, k, :8], lane_pack)
                block_pack = jnp.where(mine, block_of[t, k, :8], block_pack)
                pack = jnp.where(eight == first, east_of[t, k, :8], pack)
                pack = jnp.where(eight == first + 1, north_of[t, k, :8], pack)
            flow_lanes[t, j] = lane_pack
            flow_block[t, j] = block_pack
            flow_of[t, j] = pack
        return 0

    lax.fori_loop(0, blocks, prepare, 0)
    wet_area = area[...] * jnp.where(bot[...] > 0, 1.0, 0.0)
    vol[...] = jnp.where(eight == STEPS, wide(jnp.sum(wet_area, axis=0, keepdims=True), 8), 0.0)

    def main_copy(s, side):
        return pltpu.make_async_remote_copy(
            src_ref=out.at[s, side, pl.ds(0, 3 * rows)], dst_ref=halo.at[s, 1 - side],
            send_sem=main_send.at[s, side], recv_sem=main_recv.at[s, 1 - side],
            device_id={"space": ends[side], "level": lv}, device_id_type=pl.DeviceIdType.MESH)

    def small_copy(s, side, q, slot):
        return pltpu.make_async_remote_copy(
            src_ref=out.at[s, side, pl.ds(3 * rows, 8)], dst_ref=halo_small.at[s, 1 - side, slot],
            send_sem=hs_send.at[s, side, q], recv_sem=hs_recv.at[s, 1 - side, slot],
            device_id={"space": ends[side], "level": q}, device_id_type=pl.DeviceIdType.MESH)

    def peer_copy(s, q, slot):
        return pltpu.make_async_remote_copy(
            src_ref=small.at[s], dst_ref=peer.at[s, slot],
            send_sem=peer_send.at[s, q], recv_sem=peer_recv.at[s, slot],
            device_id={"space": sp, "level": q}, device_id_type=pl.DeviceIdType.MESH)

    def vol_copy(q, slot):
        return pltpu.make_async_remote_copy(
            src_ref=vol_line, dst_ref=vol_all.at[slot],
            send_sem=vol_send.at[q], recv_sem=vol_recv.at[slot],
            device_id={"space": q, "level": lv}, device_id_type=pl.DeviceIdType.MESH)

    others = [lax.rem(lv + d, n_level) for d in range(1, n_level)]

    def make_small(s):
        def body(t, _):
            total = jnp.sum(own[2, t] * thickness, axis=0, keepdims=True)
            flow0 = jnp.sum(own[0, t] * thickness, axis=0, keepdims=True)
            flow1 = jnp.sum(own[1, t] * thickness, axis=0, keepdims=True)
            tile = jnp.where(eight == 0, wide(flow0, 8), jnp.where(eight == 1, wide(flow1, 8), 0.0))
            tile = jnp.where(eight == 2, wide(total, 8), tile)
            small[s, t] = jnp.where(eight == 3, eta[t], tile)
            return 0
        lax.fori_loop(0, blocks, body, 0, unroll=True)

    def stage_out(s):
        for side in range(2):
            slot = wide(send[:, side * LANES:(side + 1) * LANES])
            lanes = jnp.bitwise_and(slot, LANES - 1)
            block = lax.shift_right_logical(slot, 7)
            masks = [block == b for b in range(1, blocks)]
            for g in range(3):
                out[s, side, g * rows:(g + 1) * rows] = pick([own[g, b] for b in range(blocks)], lanes, masks)
            out[s, side, 3 * rows:3 * rows + 8] = pick(
                [small[s, b] for b in range(blocks)], lanes[:8], [m[:8] for m in masks])

    def send_out(s):
        for q in others:
            peer_copy(s, q, lv).start()
        for side in range(2):
            @pl.when(has[side])
            def _():
                for q in others + [lv]:
                    small_copy(s, side, q, lv).start()
                main_copy(s, side).start()

    def gather_own():
        def body(t, _):
            tiles = [[own[g, b] for b in range(blocks)] for g in range(3)]
            for k in range(near_count):
                lanes = lanes_of[t, k]
                block = block_of[t, k]
                masks = [block == b for b in range(1, blocks)]
                for g in range(3):
                    held[t, k, g] = pick(tiles[g], lanes, masks)
            return 0
        lax.fori_loop(0, blocks, body, 0)

    def receive_small(s):
        for side in range(2):
            @pl.when(has[side])
            def _():
                for q in others + [lv]:
                    small_copy(s, 1 - side, q, q).wait_recv()

    def receive_main(s):
        for side in range(2):
            @pl.when(has[side])
            def _():
                main_copy(s, 1 - side).wait_recv()

    def close(s):
        for q in others:
            peer_copy(s, q, lv).wait_send()
        for side in range(2):
            @pl.when(has[side])
            def _():
                main_copy(s, side).wait_send()
                for q in others + [lv]:
                    small_copy(s, side, q, lv).wait_send()

    def finish_flow(slot, mine, pieces):
        total = mine
        for piece in pieces:
            total = total + piece
        flow[slot] = jnp.where(odd, wide(total[1:2], 8), wide(total[0:1], 8))

    def finish_press(slot, density, mine, pieces):
        above = jnp.zeros((1, LANES), jnp.float32)
        for q, piece in zip(others, pieces):
            above = above + jnp.where(q < lv, piece[2:3], 0.0)
        weighted = density * thickness
        column = wide(above) + running_sum(weighted, rows, row_ids) - 0.5 * weighted
        press[slot] = wide(mine[3:4]) + buoyancy * column

    def own_columns(s):
        def body(t, _):
            pieces = [peer[s, q, t] for q in others]
            finish_flow(t, small[s, t], pieces)
            finish_press(t, own[2, t], small[s, t], pieces)
            return 0
        lax.fori_loop(0, blocks, body, 0, unroll=True)

    def halo_flows(s):
        for side in range(2):
            finish_flow(blocks + side, halo_small[s, side, lv], [halo_small[s, side, q] for q in others])

    def halo_columns(s):
        for side in range(2):
            finish_press(blocks + side, halo[s, side, 2 * rows:3 * rows], halo_small[s, side, lv],
                         [halo_small[s, side, q] for q in others])

    def gather_columns():
        pressures = [press[b] for b in range(blocks)]
        flows = [flow[b] for b in range(blocks)]

        def body(t, _):
            for k in range(near_count):
                block = block_of[t, k]
                held[t, k, 3] = pick(pressures, lanes_of[t, k], [block == b for b in range(1, blocks)])
            for j in range(flow_of.shape[1]):
                block = flow_block[t, j]
                flow_held[t, j] = pick(flows, flow_lanes[t, j], [block == b for b in range(1, blocks)])
            return 0
        lax.fori_loop(0, blocks, body, 0)

    def surface(s):
        sides = [flow[blocks], flow[blocks + 1]]

        def body(t, volume):
            middle = flow[t]
            total = jnp.zeros((8, LANES), jnp.float32)
            for j in range(flow_of.shape[1]):
                lanes, block, found = flow_lanes[t, j], flow_block[t, j], flow_held[t, j]
                for side in range(2):
                    found = jnp.where(block == blocks + side, lane_gather(sides[side], lanes), found)
                total = total + flow_of[t, j] * (found - middle)
            diverge = jnp.sum(total, axis=0, keepdims=True)
            wet_node = jnp.where(bot[pl.ds(t, 1), :] > 0, 1.0, 0.0)
            part = wet_node * diverge
            eta[t] = eta[t] - time_step * wide(part, 8)
            return volume + area[pl.ds(t, 1), :] * part

        volume = lax.fori_loop(0, blocks, body, jnp.zeros((1, LANES), jnp.float32), unroll=True)
        vol[...] = jnp.where(eight == s, wide(volume, 8), vol[...])

    def advance(s):
        edges = [[halo[s, side, g * rows:(g + 1) * rows] for side in range(2)] for g in range(3)]
        edges.append([press[blocks], press[blocks + 1]])

        def body(t, _):
            here = [own[0, t], own[1, t], own[2, t], press[t]]
            zero = jnp.zeros((rows, LANES), jnp.float32)
            lap0 = lap1 = lap2 = east2 = north2 = east3 = north3 = zero
            for k in range(near_count):
                lanes = lanes_of[t, k]
                block = block_of[t, k]
                masks = [block == blocks, block == blocks + 1]
                diff = []
                for g in range(4):
                    found = held[t, k, g]
                    for side in range(2):
                        found = jnp.where(masks[side], lane_gather(edges[g][side], lanes), found)
                    diff.append(found - here[g])
                east, north, smooth = east_of[t, k], north_of[t, k], smooth_of[t, k]
                lap0 = lap0 + smooth * diff[0]
                lap1 = lap1 + smooth * diff[1]
                lap2 = lap2 + smooth * diff[2]
                east2 = east2 + east * diff[2]
                north2 = north2 + north * diff[2]
                east3 = east3 + east * diff[3]
                north3 = north3 + north * diff[3]
            bottom = wide(bot[pl.ds(t, 1), :])
            turn = wide(cor[pl.ds(t, 1), :])
            drag = jnp.where(level_ids == bottom - 1, drag_rate, 0.0)
            u, v, rho = here[:3]
            push0 = -east3 + turn * v + lap0 - drag * u
            push1 = -north3 - turn * u + lap1 - drag * v
            wet = level_ids < bottom
            own[0, t] = jnp.where(wet, u + time_step * push0, 0.0)
            own[1, t] = jnp.where(wet, v + time_step * push1, 0.0)
            own[2, t] = rho + time_step * (lap2 - u * east2 - v * north2)
            return 0
        lax.fori_loop(0, blocks, body, 0, unroll=True)

    make_small(0)
    stage_out(0)

    expected = len(row) + len(column) + low + high + (n_level - 1) * (1 + low + high)
    pl.semaphore_wait(barrier, expected)
    for q in row:
        pl.semaphore_signal(column_in, inc=1, device_id={"space": q, "level": lv})

    def step(s, _):
        send_out(s)
        gather_own()
        for q in others:
            peer_copy(s, q, q).wait_recv()
        own_columns(s)
        gather_columns()
        receive_small(s)
        halo_flows(s)
        surface(s)

        @pl.when(s == STEPS - 1)
        def _():
            sums = jnp.sum(vol[...], axis=1, keepdims=True)
            line = jnp.zeros((1, LANES), jnp.float32)
            for i in range(STEPS + 1):
                line = jnp.where(lane_ids == i, sums[i:i + 1], line)
            vol_line[...] = line
            pl.semaphore_wait(column_in, len(row))

            def start(d, _):
                vol_copy(lax.rem(sp + d, n_space), sp).start()
                return 0
            lax.fori_loop(1, n_space, start, 0)

        receive_main(s)
        halo_columns(s)
        advance(s)

        @pl.when(s < STEPS - 1)
        def _():
            make_small(s + 1)
            stage_out(s + 1)

        close(s)
        return 0

    lax.fori_loop(0, STEPS, step, 0)

    for t in range(blocks):
        here = slice(t * LANES, (t + 1) * LANES)
        vel_out[0, :, here] = own[0, t]
        vel_out[1, :, here] = own[1, t]
        den_out[:, here] = own[2, t]

    def collect(d, total):
        q = lax.rem(sp + d, n_space)
        vol_copy(q, q).wait_recv()
        return total + vol_all[q]

    total = lax.fori_loop(1, n_space, collect, vol_line[...])
    drifts = total / total[:, STEPS:STEPS + 1]
    shift = jnp.sum(jnp.where(lane_ids < STEPS, drifts, 0.0), axis=1, keepdims=True)
    for t in range(blocks):
        ele_out[t:t + 1, :] = eta[t][:1] + time_step * shift
    drift_out[...] = drifts

    def finish(d, _):
        vol_copy(lax.rem(sp + d, n_space), sp).wait_send()
        return 0

    lax.fori_loop(1, n_space, finish, 0)


def emit(vel, den, ele, drift, vel_out, den_out, ele_out, drift_out):
    vel_out[...] = vel[...]
    den_out[...] = den[...]
    ele_out[...] = ele[...]
    drift_out[...] = drift[:, :STEPS]


def solution(mesh):
    n_space, n_level = mesh.shape["space"], mesh.shape["level"]
    width = max(w for w in range(1, n_space + 1) if n_space % w == 0 and w * w <= n_space)

    def local(velocity, density, elevation, grad_weights, lap_weights, coriolis,
              node_area, thickness, send_list, neighbours, bottom):
        rows, nodes = density.shape
        blocks = nodes // LANES
        near_count = neighbours.shape[0]
        packs = -(-near_count // 4)
        f32, i32 = jnp.float32, jnp.int32
        plane = (blocks, LANES)
        vmem = pl.BlockSpec(memory_space=pltpu.VMEM)
        smem = pl.BlockSpec(memory_space=pltpu.SMEM)
        dma = pltpu.SemaphoreType.DMA
        tile = (rows, LANES)
        out = pl.pallas_call(
            functools.partial(kernel, n_space, n_level, width, rows, blocks, near_count),
            out_shape=(
                jax.ShapeDtypeStruct(velocity.shape, f32),
                jax.ShapeDtypeStruct(density.shape, f32),
                jax.ShapeDtypeStruct(plane, f32),
                jax.ShapeDtypeStruct((1, LANES), f32),
            ),
            in_specs=[vmem] * 7 + [smem] + [vmem] * 3,
            out_specs=(vmem,) * 4,
            scratch_shapes=[
                pltpu.VMEM((3, blocks) + tile, f32),
                pltpu.VMEM((blocks, 8, LANES), f32),
                pltpu.VMEM((blocks, near_count) + tile, i32),
                pltpu.VMEM((blocks, near_count) + tile, i32),
                pltpu.VMEM((blocks, near_count) + tile, f32),
                pltpu.VMEM((blocks, near_count) + tile, f32),
                pltpu.VMEM((blocks, near_count) + tile, f32),
                pltpu.VMEM((blocks, packs, 8, LANES), i32),
                pltpu.VMEM((blocks, packs, 8, LANES), i32),
                pltpu.VMEM((blocks, packs, 8, LANES), f32),
                pltpu.VMEM((blocks, near_count, 4) + tile, f32),
                pltpu.VMEM((blocks, packs, 8, LANES), f32),
                pltpu.VMEM((blocks + 2,) + tile, f32),
                pltpu.VMEM((blocks + 2, 8, LANES), f32),
                pltpu.VMEM((STEPS, blocks, 8, LANES), f32),
                pltpu.VMEM((STEPS, 2, 3 * rows + 8, LANES), f32),
                pltpu.VMEM((STEPS, 2, 3 * rows, LANES), f32),
                pltpu.VMEM((STEPS, 2, n_level, 8, LANES), f32),
                pltpu.VMEM((STEPS, n_level, blocks, 8, LANES), f32),
                pltpu.VMEM((8, LANES), f32),
                pltpu.VMEM((1, LANES), f32),
                pltpu.VMEM((n_space, 1, LANES), f32),
                dma((STEPS, 2)), dma((STEPS, 2)),
                dma((STEPS, 2, n_level)), dma((STEPS, 2, n_level)),
                dma((STEPS, n_level)), dma((STEPS, n_level)),
                dma((n_space,)), dma((n_space,)),
                pltpu.SemaphoreType.REGULAR,
            ],
            compiler_params=pltpu.CompilerParams(collective_id=0, has_side_effects=True),
        )(velocity, density, elevation.reshape(plane), grad_weights.transpose(1, 0, 2), lap_weights,
          coriolis.reshape(plane), node_area.reshape(plane), thickness, send_list,
          neighbours, bottom.reshape(plane))
        out = pl.pallas_call(
            emit,
            out_shape=(
                jax.ShapeDtypeStruct(velocity.shape, f32),
                jax.ShapeDtypeStruct(density.shape, f32),
                jax.ShapeDtypeStruct(plane, f32),
                jax.ShapeDtypeStruct((1, STEPS), f32),
            ),
            in_specs=[vmem] * 4,
            out_specs=(vmem,) * 4,
        )(*out)
        return out[0], out[1], out[2].reshape(nodes), out[3].reshape(STEPS)

    return jax.shard_map(
        local,
        mesh=mesh,
        in_specs=(
            P(None, "level", "space"),
            P("level", "space"),
            P("space"),
            P(None, None, "space"),
            P(None, "space"),
            P("space"),
            P("space"),
            P("level"),
            P("space", None),
            P(None, "space"),
            P("space"),
        ),
        out_specs=(P(None, "level", "space"), P("level", "space"), P("space"), P()),
        check_vma=False,
    )
```

```python
import functools

import jax
import jax.numpy as jnp
from jax import lax
from jax.experimental import pallas as pl
from jax.experimental.pallas import tpu as pltpu
from jax.sharding import PartitionSpec as P

STEPS = 4
LANES = 128

time_step = 0.1
buoyancy = 0.5
drag_rate = 0.5


def lane_gather(values, lanes):
    return jnp.take_along_axis(values, lanes, axis=1, mode="promise_in_bounds")


def pick(tiles, lanes, masks):
    found = lane_gather(tiles[0], lanes)
    for tile, mask in zip(tiles[1:], masks):
        found = jnp.where(mask, lane_gather(tile, lanes), found)
    return found


def running_sum(values, rows, row_ids):
    shift = 1
    while shift < rows:
        moved = pltpu.roll(values, shift, 0)
        values = values + jnp.where(row_ids >= shift, moved, 0.0)
        shift *= 2
    return values


def kernel(
    n_space, n_level, width, rows, blocks, near_count,
    vel, den, ele, grad, lap, cor, area, thick, send, near, bot,
    vel_out, den_out, ele_out, drift_out,
    own, eta, lanes_of, block_of, east_of, north_of, smooth_of,
    flow_lanes, flow_block, flow_of, held, flow_held, press, flow, small, out, halo, halo_small, peer,
    vol, vol_line, vol_all,
    main_send, main_recv, hs_send, hs_recv, peer_send, peer_recv, vol_send, vol_recv, column_in, load_sem, *loaded,
):
    sp = lax.axis_index("space")
    lv = lax.axis_index("level")
    has = (sp > 0, sp < n_space - 1)
    ends = (sp - 1, sp + 1)

    barrier = pltpu.get_barrier_semaphore()

    mine, place = sp // width, lax.rem(sp, width)
    column = [lax.rem(sp + d * width, n_space) for d in range(1, n_space // width)]
    row = [mine * width + lax.rem(place + d, width) for d in range(1, width)]
    for q in row + column:
        pl.semaphore_signal(barrier, inc=1, device_id={"space": q, "level": lv})
    for side in range(2):
        @pl.when(has[side])
        def _():
            pl.semaphore_signal(barrier, inc=1, device_id={"space": ends[side], "level": lv})
    for d in range(1, n_level):
        q = lax.rem(lv + d, n_level)
        pl.semaphore_signal(barrier, inc=1, device_id={"space": sp, "level": q})
        for side in range(2):
            @pl.when(has[side])
            def _():
                pl.semaphore_signal(barrier, inc=1, device_id={"space": ends[side], "level": q})

    loads = [
        pltpu.make_async_copy(ref, buffer, load_sem.at[i])
        for i, (ref, buffer) in enumerate(zip((vel, den, ele, grad, lap, cor, area, send, near, bot), loaded))
    ]
    for load in loads:
        load.start()
    for load in loads:
        load.wait()
    vel, den, ele, grad, lap, cor, area, send, near, bot = loaded

    row_ids = lax.broadcasted_iota(jnp.int32, (rows, LANES), 0)
    eight = lax.broadcasted_iota(jnp.int32, (8, LANES), 0)
    odd = jnp.bitwise_and(eight, 1) == 1
    lane_ids = lax.broadcasted_iota(jnp.int32, (1, LANES), 1)
    level_ids = row_ids + lv * rows
    thickness = jnp.zeros((rows, LANES), jnp.float32)
    for r in range(rows):
        thickness = jnp.where(row_ids == r, thick[r], thickness)

    def wide(row, count=rows):
        return jnp.broadcast_to(row, (count, LANES))

    low = jnp.where(has[0], 1, 0)
    high = jnp.where(has[1], 1, 0)

    def prepare(t, _):
        here = pl.ds(pl.multiple_of(t * LANES, LANES), LANES)
        bottom = wide(bot[pl.ds(t, 1), :])
        wet = level_ids < bottom
        own[0, t] = jnp.where(wet, vel[0, :, here], 0.0)
        own[1, t] = jnp.where(wet, vel[1, :, here], 0.0)
        own[2, t] = den[:, here]
        eta[t] = wide(ele[pl.ds(t, 1), :], 8)
        for k in range(near_count):
            slot = wide(near[k:k + 1, here])
            block = lax.shift_right_logical(slot, 7)
            inside = jnp.where(block < blocks, 1, jnp.where(block == blocks, low, high))
            valid = inside > 0
            lanes_of[t, k] = jnp.bitwise_and(slot, LANES - 1)
            block_of[t, k] = jnp.where(valid, block, 0)
            east = jnp.where(valid, wide(grad[k, 0:1, here]), 0.0)
            north = jnp.where(valid, wide(grad[k, 1:2, here]), 0.0)
            east_of[t, k] = east
            north_of[t, k] = north
            smooth_of[t, k] = jnp.where(valid, wide(lap[k:k + 1, here]), 0.0)
        for j in range(flow_of.shape[1]):
            lane_pack = jnp.zeros((8, LANES), jnp.int32)
            block_pack = jnp.zeros((8, LANES), jnp.int32)
            pack = jnp.zeros((8, LANES), jnp.float32)
            for k in range(4 * j, min(4 * j + 4, near_count)):
                first = 2 * (k - 4 * j)
                mine = jnp.logical_or(eight == first, eight == first + 1)
                lane_pack = jnp.where(mine, lanes_of[t, k, :8], lane_pack)
                block_pack = jnp.where(mine, block_of[t, k, :8], block_pack)
                pack = jnp.where(eight == first, east_of[t, k, :8], pack)
                pack = jnp.where(eight == first + 1, north_of[t, k, :8], pack)
            flow_lanes[t, j] = lane_pack
            flow_block[t, j] = block_pack
            flow_of[t, j] = pack
        return 0

    lax.fori_loop(0, blocks, prepare, 0)
    wet_area = area[...] * jnp.where(bot[...] > 0, 1.0, 0.0)
    vol[...] = jnp.where(eight == STEPS, wide(jnp.sum(wet_area, axis=0, keepdims=True), 8), 0.0)

    def main_copy(s, side):
        return pltpu.make_async_remote_copy(
            src_ref=out.at[s, side, pl.ds(0, 3 * rows)], dst_ref=halo.at[s, 1 - side],
            send_sem=main_send.at[s, side], recv_sem=main_recv.at[s, 1 - side],
            device_id={"space": ends[side], "level": lv}, device_id_type=pl.DeviceIdType.MESH)

    def small_copy(s, side, q, slot):
        return pltpu.make_async_remote_copy(
            src_ref=out.at[s, side, pl.ds(3 * rows, 8)], dst_ref=halo_small.at[s, 1 - side, slot],
            send_sem=hs_send.at[s, side, q], recv_sem=hs_recv.at[s, 1 - side, slot],
            device_id={"space": ends[side], "level": q}, device_id_type=pl.DeviceIdType.MESH)

    def peer_copy(s, q, slot):
        return pltpu.make_async_remote_copy(
            src_ref=small.at[s], dst_ref=peer.at[s, slot],
            send_sem=peer_send.at[s, q], recv_sem=peer_recv.at[s, slot],
            device_id={"space": sp, "level": q}, device_id_type=pl.DeviceIdType.MESH)

    def vol_copy(q, slot):
        return pltpu.make_async_remote_copy(
            src_ref=vol_line, dst_ref=vol_all.at[slot],
            send_sem=vol_send.at[q], recv_sem=vol_recv.at[slot],
            device_id={"space": q, "level": lv}, device_id_type=pl.DeviceIdType.MESH)

    others = [lax.rem(lv + d, n_level) for d in range(1, n_level)]

    def make_small(s):
        def body(t, _):
            total = jnp.sum(own[2, t] * thickness, axis=0, keepdims=True)
            flow0 = jnp.sum(own[0, t] * thickness, axis=0, keepdims=True)
            flow1 = jnp.sum(own[1, t] * thickness, axis=0, keepdims=True)
            tile = jnp.where(eight == 0, wide(flow0, 8), jnp.where(eight == 1, wide(flow1, 8), 0.0))
            tile = jnp.where(eight == 2, wide(total, 8), tile)
            small[s, t] = jnp.where(eight == 3, eta[t], tile)
            return 0
        lax.fori_loop(0, blocks, body, 0, unroll=True)

    def stage_out(s):
        for side in range(2):
            slot = wide(send[:, side * LANES:(side + 1) * LANES])
            lanes = jnp.bitwise_and(slot, LANES - 1)
            block = lax.shift_right_logical(slot, 7)
            masks = [block == b for b in range(1, blocks)]
            for g in range(3):
                out[s, side, g * rows:(g + 1) * rows] = pick([own[g, b] for b in range(blocks)], lanes, masks)
            out[s, side, 3 * rows:3 * rows + 8] = pick(
                [small[s, b] for b in range(blocks)], lanes[:8], [m[:8] for m in masks])

    def send_out(s):
        for q in others:
            peer_copy(s, q, lv).start()
        for side in range(2):
            @pl.when(has[side])
            def _():
                for q in others + [lv]:
                    small_copy(s, side, q, lv).start()
                main_copy(s, side).start()

    def gather_own():
        def body(t, _):
            tiles = [[own[g, b] for b in range(blocks)] for g in range(3)]
            for k in range(near_count):
                lanes = lanes_of[t, k]
                block = block_of[t, k]
                masks = [block == b for b in range(1, blocks)]
                for g in range(3):
                    held[t, k, g] = pick(tiles[g], lanes, masks)
            return 0
        lax.fori_loop(0, blocks, body, 0)

    def receive_small(s):
        for side in range(2):
            @pl.when(has[side])
            def _():
                for q in others + [lv]:
                    small_copy(s, 1 - side, q, q).wait_recv()

    def receive_main(s):
        for side in range(2):
            @pl.when(has[side])
            def _():
                main_copy(s, 1 - side).wait_recv()

    def close(s):
        for q in others:
            peer_copy(s, q, lv).wait_send()
        for side in range(2):
            @pl.when(has[side])
            def _():
                main_copy(s, side).wait_send()
                for q in others + [lv]:
                    small_copy(s, side, q, lv).wait_send()

    def finish_flow(slot, mine, pieces):
        total = mine
        for piece in pieces:
            total = total + piece
        flow[slot] = jnp.where(odd, wide(total[1:2], 8), wide(total[0:1], 8))

    def finish_press(slot, density, mine, pieces):
        above = jnp.zeros((1, LANES), jnp.float32)
        for q, piece in zip(others, pieces):
            above = above + jnp.where(q < lv, piece[2:3], 0.0)
        weighted = density * thickness
        column = wide(above) + running_sum(weighted, rows, row_ids) - 0.5 * weighted
        press[slot] = wide(mine[3:4]) + buoyancy * column

    def own_columns(s):
        def body(t, _):
            pieces = [peer[s, q, t] for q in others]
            finish_flow(t, small[s, t], pieces)
            finish_press(t, own[2, t], small[s, t], pieces)
            return 0
        lax.fori_loop(0, blocks, body, 0, unroll=True)

    def halo_flows(s):
        for side in range(2):
            finish_flow(blocks + side, halo_small[s, side, lv], [halo_small[s, side, q] for q in others])

    def halo_columns(s):
        for side in range(2):
            finish_press(blocks + side, halo[s, side, 2 * rows:3 * rows], halo_small[s, side, lv],
                         [halo_small[s, side, q] for q in others])

    def gather_columns():
        pressures = [press[b] for b in range(blocks)]
        flows = [flow[b] for b in range(blocks)]

        def body(t, _):
            for k in range(near_count):
                block = block_of[t, k]
                held[t, k, 3] = pick(pressures, lanes_of[t, k], [block == b for b in range(1, blocks)])
            for j in range(flow_of.shape[1]):
                block = flow_block[t, j]
                flow_held[t, j] = pick(flows, flow_lanes[t, j], [block == b for b in range(1, blocks)])
            return 0
        lax.fori_loop(0, blocks, body, 0)

    def surface(s):
        sides = [flow[blocks], flow[blocks + 1]]

        def body(t, volume):
            middle = flow[t]
            total = jnp.zeros((8, LANES), jnp.float32)
            for j in range(flow_of.shape[1]):
                lanes, block, found = flow_lanes[t, j], flow_block[t, j], flow_held[t, j]
                for side in range(2):
                    found = jnp.where(block == blocks + side, lane_gather(sides[side], lanes), found)
                total = total + flow_of[t, j] * (found - middle)
            diverge = jnp.sum(total, axis=0, keepdims=True)
            wet_node = jnp.where(bot[pl.ds(t, 1), :] > 0, 1.0, 0.0)
            part = wet_node * diverge
            eta[t] = eta[t] - time_step * wide(part, 8)
            return volume + area[pl.ds(t, 1), :] * part

        volume = lax.fori_loop(0, blocks, body, jnp.zeros((1, LANES), jnp.float32), unroll=True)
        vol[...] = jnp.where(eight == s, wide(volume, 8), vol[...])

    def advance(s):
        edges = [[halo[s, side, g * rows:(g + 1) * rows] for side in range(2)] for g in range(3)]
        edges.append([press[blocks], press[blocks + 1]])

        def body(t, _):
            here = [own[0, t], own[1, t], own[2, t], press[t]]
            zero = jnp.zeros((rows, LANES), jnp.float32)
            lap0 = lap1 = lap2 = east2 = north2 = east3 = north3 = zero
            for k in range(near_count):
                lanes = lanes_of[t, k]
                block = block_of[t, k]
                masks = [block == blocks, block == blocks + 1]
                diff = []
                for g in range(4):
                    found = held[t, k, g]
                    for side in range(2):
                        found = jnp.where(masks[side], lane_gather(edges[g][side], lanes), found)
                    diff.append(found - here[g])
                east, north, smooth = east_of[t, k], north_of[t, k], smooth_of[t, k]
                lap0 = lap0 + smooth * diff[0]
                lap1 = lap1 + smooth * diff[1]
                lap2 = lap2 + smooth * diff[2]
                east2 = east2 + east * diff[2]
                north2 = north2 + north * diff[2]
                east3 = east3 + east * diff[3]
                north3 = north3 + north * diff[3]
            bottom = wide(bot[pl.ds(t, 1), :])
            turn = wide(cor[pl.ds(t, 1), :])
            drag = jnp.where(level_ids == bottom - 1, drag_rate, 0.0)
            u, v, rho = here[:3]
            push0 = -east3 + turn * v + lap0 - drag * u
            push1 = -north3 - turn * u + lap1 - drag * v
            wet = level_ids < bottom
            own[0, t] = jnp.where(wet, u + time_step * push0, 0.0)
            own[1, t] = jnp.where(wet, v + time_step * push1, 0.0)
            own[2, t] = rho + time_step * (lap2 - u * east2 - v * north2)
            return 0
        lax.fori_loop(0, blocks, body, 0, unroll=True)

    make_small(0)
    stage_out(0)

    expected = len(row) + len(column) + low + high + (n_level - 1) * (1 + low + high)
    pl.semaphore_wait(barrier, expected)
    for q in row:
        pl.semaphore_signal(column_in, inc=1, device_id={"space": q, "level": lv})

    def step(s, _):
        send_out(s)
        gather_own()
        for q in others:
            peer_copy(s, q, q).wait_recv()
        own_columns(s)
        gather_columns()
        receive_small(s)
        halo_flows(s)
        surface(s)

        @pl.when(s == STEPS - 1)
        def _():
            sums = jnp.sum(vol[...], axis=1, keepdims=True)
            line = jnp.zeros((1, LANES), jnp.float32)
            for i in range(STEPS + 1):
                line = jnp.where(lane_ids == i, sums[i:i + 1], line)
            vol_line[...] = line
            pl.semaphore_wait(column_in, len(row))

            def start(d, _):
                vol_copy(lax.rem(sp + d, n_space), sp).start()
                return 0
            lax.fori_loop(1, n_space, start, 0)

        receive_main(s)
        halo_columns(s)
        advance(s)

        @pl.when(s < STEPS - 1)
        def _():
            make_small(s + 1)
            stage_out(s + 1)

        close(s)
        return 0

    lax.fori_loop(0, STEPS, step, 0)

    for t in range(blocks):
        here = slice(t * LANES, (t + 1) * LANES)
        vel_out[0, :, here] = own[0, t]
        vel_out[1, :, here] = own[1, t]
        den_out[:, here] = own[2, t]

    def collect(d, total):
        q = lax.rem(sp + d, n_space)
        vol_copy(q, q).wait_recv()
        return total + vol_all[q]

    total = lax.fori_loop(1, n_space, collect, vol_line[...])
    drifts = total / total[:, STEPS:STEPS + 1]
    shift = jnp.sum(jnp.where(lane_ids < STEPS, drifts, 0.0), axis=1, keepdims=True)
    for t in range(blocks):
        ele_out[t:t + 1, :] = eta[t][:1] + time_step * shift
    drift_out[...] = drifts

    def finish(d, _):
        vol_copy(lax.rem(sp + d, n_space), sp).wait_send()
        return 0

    lax.fori_loop(1, n_space, finish, 0)


def emit(vel, den, ele, drift, vel_out, den_out, ele_out, drift_out):
    vel_out[...] = vel[...]
    den_out[...] = den[...]
    ele_out[...] = ele[...]
    drift_out[...] = drift[:, :STEPS]


def solution(mesh):
    n_space, n_level = mesh.shape["space"], mesh.shape["level"]
    width = max(w for w in range(1, n_space + 1) if n_space % w == 0 and w * w <= n_space)

    def local(velocity, density, elevation, grad_weights, lap_weights, coriolis,
              node_area, thickness, send_list, neighbours, bottom):
        rows, nodes = density.shape
        blocks = nodes // LANES
        near_count = neighbours.shape[0]
        packs = -(-near_count // 4)
        f32, i32 = jnp.float32, jnp.int32
        plane = (blocks, LANES)
        vmem = pl.BlockSpec(memory_space=pltpu.VMEM)
        hbm = pl.BlockSpec(memory_space=pl.ANY)
        smem = pl.BlockSpec(memory_space=pltpu.SMEM)
        dma = pltpu.SemaphoreType.DMA
        tile = (rows, LANES)
        arrays = [velocity, density, elevation.reshape(plane), grad_weights.transpose(1, 0, 2), lap_weights,
                  coriolis.reshape(plane), node_area.reshape(plane), thickness, send_list,
                  neighbours, bottom.reshape(plane)]
        out = pl.pallas_call(
            functools.partial(kernel, n_space, n_level, width, rows, blocks, near_count),
            out_shape=(
                jax.ShapeDtypeStruct(velocity.shape, f32),
                jax.ShapeDtypeStruct(density.shape, f32),
                jax.ShapeDtypeStruct(plane, f32),
                jax.ShapeDtypeStruct((1, LANES), f32),
            ),
            in_specs=[hbm] * 7 + [smem] + [hbm] * 3,
            out_specs=(vmem,) * 4,
            scratch_shapes=[
                pltpu.VMEM((3, blocks) + tile, f32),
                pltpu.VMEM((blocks, 8, LANES), f32),
                pltpu.VMEM((blocks, near_count) + tile, i32),
                pltpu.VMEM((blocks, near_count) + tile, i32),
                pltpu.VMEM((blocks, near_count) + tile, f32),
                pltpu.VMEM((blocks, near_count) + tile, f32),
                pltpu.VMEM((blocks, near_count) + tile, f32),
                pltpu.VMEM((blocks, packs, 8, LANES), i32),
                pltpu.VMEM((blocks, packs, 8, LANES), i32),
                pltpu.VMEM((blocks, packs, 8, LANES), f32),
                pltpu.VMEM((blocks, near_count, 4) + tile, f32),
                pltpu.VMEM((blocks, packs, 8, LANES), f32),
                pltpu.VMEM((blocks + 2,) + tile, f32),
                pltpu.VMEM((blocks + 2, 8, LANES), f32),
                pltpu.VMEM((STEPS, blocks, 8, LANES), f32),
                pltpu.VMEM((STEPS, 2, 3 * rows + 8, LANES), f32),
                pltpu.VMEM((STEPS, 2, 3 * rows, LANES), f32),
                pltpu.VMEM((STEPS, 2, n_level, 8, LANES), f32),
                pltpu.VMEM((STEPS, n_level, blocks, 8, LANES), f32),
                pltpu.VMEM((8, LANES), f32),
                pltpu.VMEM((1, LANES), f32),
                pltpu.VMEM((n_space, 1, LANES), f32),
                dma((STEPS, 2)), dma((STEPS, 2)),
                dma((STEPS, 2, n_level)), dma((STEPS, 2, n_level)),
                dma((STEPS, n_level)), dma((STEPS, n_level)),
                dma((n_space,)), dma((n_space,)),
                pltpu.SemaphoreType.REGULAR,
                dma((10,)),
            ] + [pltpu.VMEM(a.shape, a.dtype) for a in arrays[:7] + arrays[8:]],
            compiler_params=pltpu.CompilerParams(collective_id=0, has_side_effects=True),
        )(*arrays)
        out = pl.pallas_call(
            emit,
            out_shape=(
                jax.ShapeDtypeStruct(velocity.shape, f32),
                jax.ShapeDtypeStruct(density.shape, f32),
                jax.ShapeDtypeStruct(plane, f32),
                jax.ShapeDtypeStruct((1, STEPS), f32),
            ),
            in_specs=[vmem] * 4,
            out_specs=(vmem,) * 4,
        )(*out)
        return out[0], out[1], out[2].reshape(nodes), out[3].reshape(STEPS)

    return jax.shard_map(
        local,
        mesh=mesh,
        in_specs=(
            P(None, "level", "space"),
            P("level", "space"),
            P("space"),
            P(None, None, "space"),
            P(None, "space"),
            P("space"),
            P("space"),
            P("level"),
            P("space", None),
            P(None, "space"),
            P("space"),
        ),
        out_specs=(P(None, "level", "space"), P("level", "space"), P("space"), P()),
        check_vma=False,
    )
```

```python
import functools

import jax
import jax.numpy as jnp
from jax import lax
from jax.experimental import pallas as pl
from jax.experimental.pallas import tpu as pltpu
from jax.sharding import PartitionSpec as P

STEPS = 4
LANES = 128

time_step = 0.1
buoyancy = 0.5
drag_rate = 0.5


def lane_gather(values, lanes):
    return jnp.take_along_axis(values, lanes, axis=1, mode="promise_in_bounds")


def pick(tiles, lanes, masks):
    found = lane_gather(tiles[0], lanes)
    for tile, mask in zip(tiles[1:], masks):
        found = jnp.where(mask, lane_gather(tile, lanes), found)
    return found


def running_sum(values, rows, row_ids):
    shift = 1
    while shift < rows:
        moved = pltpu.roll(values, shift, 0)
        values = values + jnp.where(row_ids >= shift, moved, 0.0)
        shift *= 2
    return values


def kernel(
    n_space, n_level, width, rows, blocks, near_count,
    vel, den, ele, grad, lap, cor, area, thick, send, near, bot,
    vel_out, den_out, ele_out, drift_out,
    own, eta, lanes_of, block_of, east_of, north_of, smooth_of,
    flow_lanes, flow_block, flow_of, held, flow_held, press, flow, small, out, halo, halo_small, peer,
    vol, vol_line, vol_all,
    main_send, main_recv, hs_send, hs_recv, peer_send, peer_recv, vol_send, vol_recv, column_in, load_sem, vel_held, den_held, store_sem, *loaded,
):
    sp = lax.axis_index("space")
    lv = lax.axis_index("level")
    has = (sp > 0, sp < n_space - 1)
    ends = (sp - 1, sp + 1)

    barrier = pltpu.get_barrier_semaphore()

    mine, place = sp // width, lax.rem(sp, width)
    column = [lax.rem(sp + d * width, n_space) for d in range(1, n_space // width)]
    row = [mine * width + lax.rem(place + d, width) for d in range(1, width)]
    for q in row + column:
        pl.semaphore_signal(barrier, inc=1, device_id={"space": q, "level": lv})
    for side in range(2):
        @pl.when(has[side])
        def _():
            pl.semaphore_signal(barrier, inc=1, device_id={"space": ends[side], "level": lv})
    for d in range(1, n_level):
        q = lax.rem(lv + d, n_level)
        pl.semaphore_signal(barrier, inc=1, device_id={"space": sp, "level": q})
        for side in range(2):
            @pl.when(has[side])
            def _():
                pl.semaphore_signal(barrier, inc=1, device_id={"space": ends[side], "level": q})

    loads = [
        pltpu.make_async_copy(ref, buffer, load_sem.at[i])
        for i, (ref, buffer) in enumerate(zip((vel, den, ele, grad, lap, cor, area, send, near, bot), loaded))
    ]
    for load in loads:
        load.start()
    for load in loads:
        load.wait()
    vel, den, ele, grad, lap, cor, area, send, near, bot = loaded

    row_ids = lax.broadcasted_iota(jnp.int32, (rows, LANES), 0)
    eight = lax.broadcasted_iota(jnp.int32, (8, LANES), 0)
    odd = jnp.bitwise_and(eight, 1) == 1
    lane_ids = lax.broadcasted_iota(jnp.int32, (1, LANES), 1)
    level_ids = row_ids + lv * rows
    thickness = jnp.zeros((rows, LANES), jnp.float32)
    for r in range(rows):
        thickness = jnp.where(row_ids == r, thick[r], thickness)

    def wide(row, count=rows):
        return jnp.broadcast_to(row, (count, LANES))

    low = jnp.where(has[0], 1, 0)
    high = jnp.where(has[1], 1, 0)

    def prepare(t, _):
        here = pl.ds(pl.multiple_of(t * LANES, LANES), LANES)
        bottom = wide(bot[pl.ds(t, 1), :])
        wet = level_ids < bottom
        own[0, t] = jnp.where(wet, vel[0, :, here], 0.0)
        own[1, t] = jnp.where(wet, vel[1, :, here], 0.0)
        own[2, t] = den[:, here]
        eta[t] = wide(ele[pl.ds(t, 1), :], 8)
        for k in range(near_count):
            slot = wide(near[k:k + 1, here])
            block = lax.shift_right_logical(slot, 7)
            inside = jnp.where(block < blocks, 1, jnp.where(block == blocks, low, high))
            valid = inside > 0
            lanes_of[t, k] = jnp.bitwise_and(slot, LANES - 1)
            block_of[t, k] = jnp.where(valid, block, 0)
            east = jnp.where(valid, wide(grad[k, 0:1, here]), 0.0)
            north = jnp.where(valid, wide(grad[k, 1:2, here]), 0.0)
            east_of[t, k] = east
            north_of[t, k] = north
            smooth_of[t, k] = jnp.where(valid, wide(lap[k:k + 1, here]), 0.0)
        for j in range(flow_of.shape[1]):
            lane_pack = jnp.zeros((8, LANES), jnp.int32)
            block_pack = jnp.zeros((8, LANES), jnp.int32)
            pack = jnp.zeros((8, LANES), jnp.float32)
            for k in range(4 * j, min(4 * j + 4, near_count)):
                first = 2 * (k - 4 * j)
                mine = jnp.logical_or(eight == first, eight == first + 1)
                lane_pack = jnp.where(mine, lanes_of[t, k, :8], lane_pack)
                block_pack = jnp.where(mine, block_of[t, k, :8], block_pack)
                pack = jnp.where(eight == first, east_of[t, k, :8], pack)
                pack = jnp.where(eight == first + 1, north_of[t, k, :8], pack)
            flow_lanes[t, j] = lane_pack
            flow_block[t, j] = block_pack
            flow_of[t, j] = pack
        return 0

    lax.fori_loop(0, blocks, prepare, 0)
    wet_area = area[...] * jnp.where(bot[...] > 0, 1.0, 0.0)
    vol[...] = jnp.where(eight == STEPS, wide(jnp.sum(wet_area, axis=0, keepdims=True), 8), 0.0)

    def main_copy(s, side):
        return pltpu.make_async_remote_copy(
            src_ref=out.at[s, side, pl.ds(0, 3 * rows)], dst_ref=halo.at[s, 1 - side],
            send_sem=main_send.at[s, side], recv_sem=main_recv.at[s, 1 - side],
            device_id={"space": ends[side], "level": lv}, device_id_type=pl.DeviceIdType.MESH)

    def small_copy(s, side, q, slot):
        return pltpu.make_async_remote_copy(
            src_ref=out.at[s, side, pl.ds(3 * rows, 8)], dst_ref=halo_small.at[s, 1 - side, slot],
            send_sem=hs_send.at[s, side, q], recv_sem=hs_recv.at[s, 1 - side, slot],
            device_id={"space": ends[side], "level": q}, device_id_type=pl.DeviceIdType.MESH)

    def peer_copy(s, q, slot):
        return pltpu.make_async_remote_copy(
            src_ref=small.at[s], dst_ref=peer.at[s, slot],
            send_sem=peer_send.at[s, q], recv_sem=peer_recv.at[s, slot],
            device_id={"space": sp, "level": q}, device_id_type=pl.DeviceIdType.MESH)

    def vol_copy(q, slot):
        return pltpu.make_async_remote_copy(
            src_ref=vol_line, dst_ref=vol_all.at[slot],
            send_sem=vol_send.at[q], recv_sem=vol_recv.at[slot],
            device_id={"space": q, "level": lv}, device_id_type=pl.DeviceIdType.MESH)

    others = [lax.rem(lv + d, n_level) for d in range(1, n_level)]

    def make_small(s):
        def body(t, _):
            total = jnp.sum(own[2, t] * thickness, axis=0, keepdims=True)
            flow0 = jnp.sum(own[0, t] * thickness, axis=0, keepdims=True)
            flow1 = jnp.sum(own[1, t] * thickness, axis=0, keepdims=True)
            tile = jnp.where(eight == 0, wide(flow0, 8), jnp.where(eight == 1, wide(flow1, 8), 0.0))
            tile = jnp.where(eight == 2, wide(total, 8), tile)
            small[s, t] = jnp.where(eight == 3, eta[t], tile)
            return 0
        lax.fori_loop(0, blocks, body, 0, unroll=True)

    def stage_out(s):
        for side in range(2):
            slot = wide(send[:, side * LANES:(side + 1) * LANES])
            lanes = jnp.bitwise_and(slot, LANES - 1)
            block = lax.shift_right_logical(slot, 7)
            masks = [block == b for b in range(1, blocks)]
            for g in range(3):
                out[s, side, g * rows:(g + 1) * rows] = pick([own[g, b] for b in range(blocks)], lanes, masks)
            out[s, side, 3 * rows:3 * rows + 8] = pick(
                [small[s, b] for b in range(blocks)], lanes[:8], [m[:8] for m in masks])

    def send_out(s):
        for q in others:
            peer_copy(s, q, lv).start()
        for side in range(2):
            @pl.when(has[side])
            def _():
                for q in others + [lv]:
                    small_copy(s, side, q, lv).start()
                main_copy(s, side).start()

    def gather_own():
        def body(t, _):
            tiles = [[own[g, b] for b in range(blocks)] for g in range(3)]
            for k in range(near_count):
                lanes = lanes_of[t, k]
                block = block_of[t, k]
                masks = [block == b for b in range(1, blocks)]
                for g in range(3):
                    held[t, k, g] = pick(tiles[g], lanes, masks)
            return 0
        lax.fori_loop(0, blocks, body, 0)

    def receive_small(s):
        for side in range(2):
            @pl.when(has[side])
            def _():
                for q in others + [lv]:
                    small_copy(s, 1 - side, q, q).wait_recv()

    def receive_main(s):
        for side in range(2):
            @pl.when(has[side])
            def _():
                main_copy(s, 1 - side).wait_recv()

    def close(s):
        for q in others:
            peer_copy(s, q, lv).wait_send()
        for side in range(2):
            @pl.when(has[side])
            def _():
                main_copy(s, side).wait_send()
                for q in others + [lv]:
                    small_copy(s, side, q, lv).wait_send()

    def finish_flow(slot, mine, pieces):
        total = mine
        for piece in pieces:
            total = total + piece
        flow[slot] = jnp.where(odd, wide(total[1:2], 8), wide(total[0:1], 8))

    def finish_press(slot, density, mine, pieces):
        above = jnp.zeros((1, LANES), jnp.float32)
        for q, piece in zip(others, pieces):
            above = above + jnp.where(q < lv, piece[2:3], 0.0)
        weighted = density * thickness
        column = wide(above) + running_sum(weighted, rows, row_ids) - 0.5 * weighted
        press[slot] = wide(mine[3:4]) + buoyancy * column

    def own_columns(s):
        def body(t, _):
            pieces = [peer[s, q, t] for q in others]
            finish_flow(t, small[s, t], pieces)
            finish_press(t, own[2, t], small[s, t], pieces)
            return 0
        lax.fori_loop(0, blocks, body, 0, unroll=True)

    def halo_flows(s):
        for side in range(2):
            finish_flow(blocks + side, halo_small[s, side, lv], [halo_small[s, side, q] for q in others])

    def halo_columns(s):
        for side in range(2):
            finish_press(blocks + side, halo[s, side, 2 * rows:3 * rows], halo_small[s, side, lv],
                         [halo_small[s, side, q] for q in others])

    def gather_columns():
        pressures = [press[b] for b in range(blocks)]
        flows = [flow[b] for b in range(blocks)]

        def body(t, _):
            for k in range(near_count):
                block = block_of[t, k]
                held[t, k, 3] = pick(pressures, lanes_of[t, k], [block == b for b in range(1, blocks)])
            for j in range(flow_of.shape[1]):
                block = flow_block[t, j]
                flow_held[t, j] = pick(flows, flow_lanes[t, j], [block == b for b in range(1, blocks)])
            return 0
        lax.fori_loop(0, blocks, body, 0)

    def surface(s):
        sides = [flow[blocks], flow[blocks + 1]]

        def body(t, volume):
            middle = flow[t]
            total = jnp.zeros((8, LANES), jnp.float32)
            for j in range(flow_of.shape[1]):
                lanes, block, found = flow_lanes[t, j], flow_block[t, j], flow_held[t, j]
                for side in range(2):
                    found = jnp.where(block == blocks + side, lane_gather(sides[side], lanes), found)
                total = total + flow_of[t, j] * (found - middle)
            diverge = jnp.sum(total, axis=0, keepdims=True)
            wet_node = jnp.where(bot[pl.ds(t, 1), :] > 0, 1.0, 0.0)
            part = wet_node * diverge
            eta[t] = eta[t] - time_step * wide(part, 8)
            return volume + area[pl.ds(t, 1), :] * part

        volume = lax.fori_loop(0, blocks, body, jnp.zeros((1, LANES), jnp.float32), unroll=True)
        vol[...] = jnp.where(eight == s, wide(volume, 8), vol[...])

    def advance(s):
        edges = [[halo[s, side, g * rows:(g + 1) * rows] for side in range(2)] for g in range(3)]
        edges.append([press[blocks], press[blocks + 1]])

        def body(t, _):
            here = [own[0, t], own[1, t], own[2, t], press[t]]
            zero = jnp.zeros((rows, LANES), jnp.float32)
            lap0 = lap1 = lap2 = east2 = north2 = east3 = north3 = zero
            for k in range(near_count):
                lanes = lanes_of[t, k]
                block = block_of[t, k]
                masks = [block == blocks, block == blocks + 1]
                diff = []
                for g in range(4):
                    found = held[t, k, g]
                    for side in range(2):
                        found = jnp.where(masks[side], lane_gather(edges[g][side], lanes), found)
                    diff.append(found - here[g])
                east, north, smooth = east_of[t, k], north_of[t, k], smooth_of[t, k]
                lap0 = lap0 + smooth * diff[0]
                lap1 = lap1 + smooth * diff[1]
                lap2 = lap2 + smooth * diff[2]
                east2 = east2 + east * diff[2]
                north2 = north2 + north * diff[2]
                east3 = east3 + east * diff[3]
                north3 = north3 + north * diff[3]
            bottom = wide(bot[pl.ds(t, 1), :])
            turn = wide(cor[pl.ds(t, 1), :])
            drag = jnp.where(level_ids == bottom - 1, drag_rate, 0.0)
            u, v, rho = here[:3]
            push0 = -east3 + turn * v + lap0 - drag * u
            push1 = -north3 - turn * u + lap1 - drag * v
            wet = level_ids < bottom
            own[0, t] = jnp.where(wet, u + time_step * push0, 0.0)
            own[1, t] = jnp.where(wet, v + time_step * push1, 0.0)
            own[2, t] = rho + time_step * (lap2 - u * east2 - v * north2)
            return 0
        lax.fori_loop(0, blocks, body, 0, unroll=True)

    make_small(0)
    stage_out(0)

    expected = len(row) + len(column) + low + high + (n_level - 1) * (1 + low + high)
    pl.semaphore_wait(barrier, expected)
    for q in row:
        pl.semaphore_signal(column_in, inc=1, device_id={"space": q, "level": lv})

    def step(s, _):
        send_out(s)
        gather_own()
        for q in others:
            peer_copy(s, q, q).wait_recv()
        own_columns(s)
        gather_columns()
        receive_small(s)
        halo_flows(s)
        surface(s)

        @pl.when(s == STEPS - 1)
        def _():
            sums = jnp.sum(vol[...], axis=1, keepdims=True)
            line = jnp.zeros((1, LANES), jnp.float32)
            for i in range(STEPS + 1):
                line = jnp.where(lane_ids == i, sums[i:i + 1], line)
            vol_line[...] = line
            pl.semaphore_wait(column_in, len(row))

            def start(d, _):
                vol_copy(lax.rem(sp + d, n_space), sp).start()
                return 0
            lax.fori_loop(1, n_space, start, 0)

        receive_main(s)
        halo_columns(s)
        advance(s)

        @pl.when(s < STEPS - 1)
        def _():
            make_small(s + 1)
            stage_out(s + 1)

        close(s)
        return 0

    lax.fori_loop(0, STEPS, step, 0)

    for t in range(blocks):
        here = slice(t * LANES, (t + 1) * LANES)
        vel_held[0, :, here] = own[0, t]
        vel_held[1, :, here] = own[1, t]
        den_held[:, here] = own[2, t]

    def collect(d, total):
        q = lax.rem(sp + d, n_space)
        vol_copy(q, q).wait_recv()
        return total + vol_all[q]

    total = collect(1, vol_line[...])
    stores = [pltpu.make_async_copy(vel_held, vel_out, store_sem.at[0]),
              pltpu.make_async_copy(den_held, den_out, store_sem.at[1])]
    for store in stores:
        store.start()
    total = lax.fori_loop(2, n_space, collect, total)
    drifts = total / total[:, STEPS:STEPS + 1]
    shift = jnp.sum(jnp.where(lane_ids < STEPS, drifts, 0.0), axis=1, keepdims=True)
    for t in range(blocks):
        ele_out[t:t + 1, :] = eta[t][:1] + time_step * shift
    drift_out[...] = drifts
    for store in stores:
        store.wait()

    def finish(d, _):
        vol_copy(lax.rem(sp + d, n_space), sp).wait_send()
        return 0

    lax.fori_loop(1, n_space, finish, 0)


def emit(vel, den, ele, drift, vel_out, den_out, ele_out, drift_out):
    vel_out[...] = vel[...]
    den_out[...] = den[...]
    ele_out[...] = ele[...]
    drift_out[...] = drift[:, :STEPS]


def solution(mesh):
    n_space, n_level = mesh.shape["space"], mesh.shape["level"]
    width = max(w for w in range(1, n_space + 1) if n_space % w == 0 and w * w <= n_space)

    def local(velocity, density, elevation, grad_weights, lap_weights, coriolis,
              node_area, thickness, send_list, neighbours, bottom):
        rows, nodes = density.shape
        blocks = nodes // LANES
        near_count = neighbours.shape[0]
        packs = -(-near_count // 4)
        f32, i32 = jnp.float32, jnp.int32
        plane = (blocks, LANES)
        vmem = pl.BlockSpec(memory_space=pltpu.VMEM)
        hbm = pl.BlockSpec(memory_space=pl.ANY)
        smem = pl.BlockSpec(memory_space=pltpu.SMEM)
        dma = pltpu.SemaphoreType.DMA
        tile = (rows, LANES)
        arrays = [velocity, density, elevation.reshape(plane), grad_weights.transpose(1, 0, 2), lap_weights,
                  coriolis.reshape(plane), node_area.reshape(plane), thickness, send_list,
                  neighbours, bottom.reshape(plane)]
        out = pl.pallas_call(
            functools.partial(kernel, n_space, n_level, width, rows, blocks, near_count),
            out_shape=(
                jax.ShapeDtypeStruct(velocity.shape, f32),
                jax.ShapeDtypeStruct(density.shape, f32),
                jax.ShapeDtypeStruct(plane, f32),
                jax.ShapeDtypeStruct((1, LANES), f32),
            ),
            in_specs=[hbm] * 7 + [smem] + [hbm] * 3,
            out_specs=(hbm, hbm, vmem, vmem),
            scratch_shapes=[
                pltpu.VMEM((3, blocks) + tile, f32),
                pltpu.VMEM((blocks, 8, LANES), f32),
                pltpu.VMEM((blocks, near_count) + tile, i32),
                pltpu.VMEM((blocks, near_count) + tile, i32),
                pltpu.VMEM((blocks, near_count) + tile, f32),
                pltpu.VMEM((blocks, near_count) + tile, f32),
                pltpu.VMEM((blocks, near_count) + tile, f32),
                pltpu.VMEM((blocks, packs, 8, LANES), i32),
                pltpu.VMEM((blocks, packs, 8, LANES), i32),
                pltpu.VMEM((blocks, packs, 8, LANES), f32),
                pltpu.VMEM((blocks, near_count, 4) + tile, f32),
                pltpu.VMEM((blocks, packs, 8, LANES), f32),
                pltpu.VMEM((blocks + 2,) + tile, f32),
                pltpu.VMEM((blocks + 2, 8, LANES), f32),
                pltpu.VMEM((STEPS, blocks, 8, LANES), f32),
                pltpu.VMEM((STEPS, 2, 3 * rows + 8, LANES), f32),
                pltpu.VMEM((STEPS, 2, 3 * rows, LANES), f32),
                pltpu.VMEM((STEPS, 2, n_level, 8, LANES), f32),
                pltpu.VMEM((STEPS, n_level, blocks, 8, LANES), f32),
                pltpu.VMEM((8, LANES), f32),
                pltpu.VMEM((1, LANES), f32),
                pltpu.VMEM((n_space, 1, LANES), f32),
                dma((STEPS, 2)), dma((STEPS, 2)),
                dma((STEPS, 2, n_level)), dma((STEPS, 2, n_level)),
                dma((STEPS, n_level)), dma((STEPS, n_level)),
                dma((n_space,)), dma((n_space,)),
                pltpu.SemaphoreType.REGULAR,
                dma((10,)),
                pltpu.VMEM(velocity.shape, f32),
                pltpu.VMEM(density.shape, f32),
                dma((2,)),
            ] + [pltpu.VMEM(a.shape, a.dtype) for a in arrays[:7] + arrays[8:]],
            compiler_params=pltpu.CompilerParams(collective_id=0, has_side_effects=True),
        )(*arrays)
        out = pl.pallas_call(
            emit,
            out_shape=(
                jax.ShapeDtypeStruct(velocity.shape, f32),
                jax.ShapeDtypeStruct(density.shape, f32),
                jax.ShapeDtypeStruct(plane, f32),
                jax.ShapeDtypeStruct((1, STEPS), f32),
            ),
            in_specs=[vmem] * 4,
            out_specs=(vmem,) * 4,
        )(*out)
        return out[0], out[1], out[2].reshape(nodes), out[3].reshape(STEPS)

    return jax.shard_map(
        local,
        mesh=mesh,
        in_specs=(
            P(None, "level", "space"),
            P("level", "space"),
            P("space"),
            P(None, None, "space"),
            P(None, "space"),
            P("space"),
            P("space"),
            P("level"),
            P("space", None),
            P(None, "space"),
            P("space"),
        ),
        out_specs=(P(None, "level", "space"), P("level", "space"), P("space"), P()),
        check_vma=False,
    )
```
